256 devices in a mesh: tm: 128 (over z, y, x), tensor: 2 (over core).
Axes of the slice: x: 4, y: 4, z: 8, core: 2. Of those that a mesh axis runs over, the one named last changes fastest.
Arguments:
- noise_start: float32 [1, 16384], replicated, may hold values from -6 to 6
- timesteps: int32 [129], replicated, may hold values from 0 to 599, as said below
- class_labels: int32 [128, 1], P('tm'), may hold values from 0 to 999
- mixing: float32 [2, 128], P(None, 'tm'), may hold values from -0.5 to 0.5
- class_table: bfloat16 [1000, 768], replicated, may hold values from -3 to 3
- time_in: bfloat16 [256, 768], replicated, may hold values from -0.75 to 0.75
- time_out: bfloat16 [768, 768], replicated, may hold values from -0.21875 to 0.21875
- ada_weight: bfloat16 [768, 4608], replicated, may hold values from -0.21875 to 0.21875
- final_ada: bfloat16 [768, 1536], replicated, may hold values from -0.21875 to 0.21875
- patch_weight: bfloat16 [16, 768], replicated, may hold values from -1.5 to 1.5
- q_weight: bfloat16 [768, 768], replicated, may hold values from -1.5 to 1.5
- kv_weight: bfloat16 [768, 1536], replicated, may hold values from -1.5 to 1.5
- out_weight: bfloat16 [768, 768], replicated, may hold values from -0.4375 to 0.4375
- up_weight: bfloat16 [768, 3072], P(None, 'tensor'), may hold values from -0.21875 to 0.21875
- down_weight: bfloat16 [3072, 768], P('tensor'), may hold values from -0.21875 to 0.21875
- final_weight: bfloat16 [768, 16], replicated, may hold values from -0.21875 to 0.21875
Outputs:
- states: float32 [128, 1, 16384], P('tm')
- residuals: float32 [2, 128], P(None, 'tm')
The draws below stay inside these ranges and needn't reach their ends.
Inputs may be any that keep to these rules, and one draw needn't show every extreme that they name: `timesteps`: strictly decreasing; the first is 599, the last is 0, all others lie from 100 to 549.
All inputs are finite; a program needn't handle non-finite values.
Results may differ from the reference program's by a relative error of at most 0.008.
Values may be sent and summed in bfloat16 or wider, within the bound.
No kernel may reach another device: no remote copies, remote signals or barrier semaphores. Data moves between devices by JAX's collectives and lax.ppermute only.
A program may use at most 128 MiB of HBM per device.

```python
import math
import jax
import jax.numpy as jnp
from jax import lax

D = 768
HEADS = 12
FF = 3072
SEQ = 1024
PATCH = 16
CLASSES = 1000
FREQ = 256
IMG = 1
ITERS = 2
WINDOW = 128
LAT = 16384
N_TENSOR = 2


def attention_pair(key):
    query_key = jax.random.fold_in(key, 101)
    other_key = jax.random.fold_in(key, 202)
    query_part = jax.random.normal(query_key, (D, D), jnp.float32) / jnp.sqrt(jnp.float32(D))
    key_part = jax.random.normal(other_key, (D, 2 * D), jnp.float32) / jnp.sqrt(jnp.float32(D))
    head_width = D // HEADS
    head_rank = jax.random.permutation(jax.random.fold_in(key, 303), HEADS)
    chosen = (head_rank < HEADS // 2).astype(jnp.float32)
    strength = 1.5
    column_head = jnp.arange(D, dtype=jnp.int32) // head_width
    column_match = (column_head[:, None] == jnp.arange(HEADS, dtype=jnp.int32)[None, :]).astype(jnp.float32)
    factor = strength * jnp.sum(column_match * chosen[None, :], axis=1)
    keys = key_part[:, :D] + factor[None, :] * query_part
    key_part = jnp.concatenate([keys, key_part[:, D:]], axis=1)
    return (jnp.clip(query_part, -1.5, 1.5), jnp.clip(key_part, -1.5, 1.5))


def draw_q_weight(key, part):
    return attention_pair(key)[0].astype(jnp.bfloat16)


def draw_kv_weight(key, part):
    return attention_pair(key)[1].astype(jnp.bfloat16)


def draw_timesteps(key, part):
    chosen = jax.random.permutation(key, 450)[:WINDOW - 1].astype(jnp.int32) + 100
    lower = -jnp.sort(-chosen)
    return jnp.concatenate([jnp.full((1,), 599, jnp.int32), lower, jnp.zeros((1,), jnp.int32)])


def plant(entries, key, low, high):
    place = [jax.random.randint(jax.random.fold_in(key, axis), (), 0, length) for axis, length in enumerate(entries.shape)]
    longest = entries.shape.index(max(entries.shape))
    beside = place[:longest] + [(place[longest] + 1) % entries.shape[longest]] + place[longest + 1:]
    return entries.at[tuple(place)].set(low).at[tuple(beside)].set(high)


def block_scale(rng, shape, shards, least, largest):
    gain = 1.0
    for axis_at, parts in shards:
        steps = jax.random.uniform(jax.random.fold_in(jax.random.fold_in(rng, 6), axis_at), (parts,), jnp.float32, least / len(shards), largest / len(shards))
        gain = gain * jnp.repeat(jnp.exp(steps), shape[axis_at] // parts).reshape((-1,) + (1,) * (len(shape) - 1 - axis_at))
    return gain


def gaussian(stream_key, extent, scale, reach, shards=(), kind=jnp.bfloat16):
    factor_of = block_scale(stream_key, extent, shards, -0.22, 0.18) if shards else 1.0
    result = jax.random.normal(stream_key, extent, jnp.float32) * scale * factor_of
    return jnp.minimum(jnp.maximum(result, -reach), reach).astype(kind)


def setup_inputs(seed: int = 0) -> dict:
    seeds = jax.random.split(jax.random.key(seed), 17)
    noise_start = gaussian(seeds[0], (IMG, LAT), 1.0, 6.0, (), jnp.float32)
    timesteps = draw_timesteps(jax.random.fold_in(seeds[16], 71), 0)
    class_labels = plant(jax.random.randint(seeds[2], (WINDOW, IMG), 0, CLASSES), jax.random.fold_in(seeds[2], 1), 0, CLASSES - 1).astype(jnp.int32)
    mixing = jnp.clip(jax.random.uniform(seeds[3], (ITERS, WINDOW), jnp.float32, -0.5, 0.5) * block_scale(seeds[3], (ITERS, WINDOW), ((1, 128),), -0.4, 0.0), -0.5, 0.5)
    class_table = gaussian(seeds[4], (CLASSES, D), 0.5, 3.0)
    time_in = gaussian(seeds[5], (FREQ, D), (FREQ // 4) ** -0.5, 0.75)
    time_out = gaussian(seeds[6], (D, D), D ** -0.5, 0.21875)
    ada_weight = gaussian(seeds[7], (D, 6 * D), D ** -0.5, 0.21875)
    final_ada = gaussian(seeds[8], (D, 2 * D), D ** -0.5, 0.21875)
    patch_weight = gaussian(seeds[9], (PATCH, D), PATCH ** -0.5, 1.5)
    q_weight = draw_q_weight(jax.random.fold_in(seeds[16], 71), 0)
    kv_weight = draw_kv_weight(jax.random.fold_in(seeds[16], 71), 0)
    out_weight = gaussian(seeds[12], (D, D), (D // 4) ** -0.5, 0.4375)
    up_weight = gaussian(seeds[13], (D, FF), D ** -0.5, 0.21875, ((1, 2),))
    down_weight = gaussian(seeds[14], (FF, D), (FF // 4) ** -0.5, 0.21875, ((0, 2),))
    final_weight = gaussian(seeds[15], (D, PATCH), D ** -0.5, 0.21875)
    return {"noise_start": noise_start, "timesteps": timesteps, "class_labels": class_labels, "mixing": mixing, "class_table": class_table, "time_in": time_in, "time_out": time_out, "ada_weight": ada_weight, "final_ada": final_ada, "patch_weight": patch_weight, "q_weight": q_weight, "kv_weight": kv_weight, "out_weight": out_weight, "up_weight": up_weight, "down_weight": down_weight, "final_weight": final_weight}


norm_eps = 1e-06
plan_steps = 1000

def log_table():
    levels = jnp.arange(plan_steps, dtype=jnp.float32)
    beta_values = 0.0001 + (0.02 - 0.0001) * levels / (plan_steps - 1)
    return jnp.cumsum(jnp.log(1.0 - beta_values))

def alpha_at(moments):
    matches = moments[:, None] == jnp.arange(plan_steps, dtype=jnp.int32)[None, :]
    return jnp.exp(lax.optimization_barrier(jnp.sum(jnp.where(matches, log_table()[None, :], 0.0), axis=1)))

def time_features(moment):
    half_count = FREQ // 2
    freq_rates = jnp.exp(-math.log(10000.0) * jnp.arange(half_count, dtype=jnp.float32) / half_count)
    angles = moment.astype(jnp.float32) * freq_rates
    return jnp.concatenate([jnp.cos(angles), jnp.sin(angles)])[None, :]

def positions():
    half_width = D // 2
    places = jnp.arange(SEQ, dtype=jnp.float32)[:, None]
    freq_rates = jnp.exp(-math.log(10000.0) * jnp.arange(half_width, dtype=jnp.float32) / half_width)
    angles = places * freq_rates[None, :]
    return jnp.concatenate([jnp.sin(angles), jnp.cos(angles)], axis=1)

def layer_norm(values):
    center = values - lax.optimization_barrier(jnp.mean(values, axis=-1, keepdims=True))
    spread = lax.optimization_barrier(jnp.mean(center * center, axis=-1, keepdims=True))
    return center * lax.rsqrt(spread + norm_eps)

def modulate(values, shift, scale):
    return layer_norm(values) * (1.0 + scale) + shift

def split_rows(matrix, count):
    return [matrix[:, None, column * D:(column + 1) * D] for column in range(count)]

def condition(moment, labels, class_table, time_in, time_out, ada_weight, final_ada):
    features = time_features(moment).astype(jnp.bfloat16)
    time_hidden = jax.nn.silu(jnp.dot(features, time_in, preferred_element_type=jnp.float32)).astype(jnp.bfloat16)
    time_embed = jnp.dot(time_hidden, time_out, preferred_element_type=jnp.float32)
    onehot = (labels[:, None] == jnp.arange(CLASSES, dtype=jnp.int32)[None, :]).astype(jnp.bfloat16)
    classes = jnp.dot(onehot, class_table, preferred_element_type=jnp.float32)
    summed = jax.nn.silu(time_embed + classes).astype(jnp.bfloat16)
    modul = jnp.dot(summed, ada_weight, preferred_element_type=jnp.float32)
    final_mod = jnp.dot(summed, final_ada, preferred_element_type=jnp.float32)
    return (modul, final_mod)

def denoise(state_in, moment, labels, params):
    class_table, time_in, time_out, ada_weight, final_ada, patch_weight, q_weight, kv_weight, out_weight, up_weight, down_weight, final_weight = params
    modul, final_mod = condition(moment, labels, class_table, time_in, time_out, ada_weight, final_ada)
    shift_attn, scale_attn, gate_attn, shift_mlp, scale_mlp, gate_mlp = split_rows(modul, 6)
    shift_out, scale_out = split_rows(final_mod, 2)
    head_dim = D // HEADS
    tokens = state_in.astype(jnp.bfloat16).reshape(IMG * SEQ, PATCH)
    hidden = jnp.dot(tokens, patch_weight, preferred_element_type=jnp.float32).reshape(IMG, SEQ, D) + positions()[None]
    attn_in = modulate(hidden, shift_attn, scale_attn).astype(jnp.bfloat16).reshape(IMG * SEQ, D)
    queries = jnp.dot(attn_in, q_weight, preferred_element_type=jnp.float32).astype(jnp.bfloat16)
    queries = queries.reshape(IMG, SEQ, HEADS, head_dim)
    key_value = jnp.dot(attn_in, kv_weight, preferred_element_type=jnp.float32).astype(jnp.bfloat16)
    key_value = key_value.reshape(IMG, SEQ, 2 * D)
    key_heads = key_value[:, :, :D].reshape(IMG, SEQ, HEADS, head_dim)
    value_heads = key_value[:, :, D:].reshape(IMG, SEQ, HEADS, head_dim)
    scores = jnp.einsum('bqhd,bkhd->bhqk', queries.astype(jnp.float32), key_heads.astype(jnp.float32))
    scores = scores * (1.0 / math.sqrt(head_dim))
    attention = jax.nn.softmax(scores, axis=-1).astype(jnp.bfloat16)
    attended = jnp.einsum('bhqk,bkhd->bqhd', attention.astype(jnp.float32), value_heads.astype(jnp.float32))
    attended = attended.astype(jnp.bfloat16).reshape(IMG * SEQ, D)
    hidden = hidden + gate_attn * jnp.dot(attended, out_weight, preferred_element_type=jnp.float32).reshape(IMG, SEQ, D)
    mlp_in = modulate(hidden, shift_mlp, scale_mlp).astype(jnp.bfloat16).reshape(IMG * SEQ, D)
    lifted = jax.nn.gelu(jnp.dot(mlp_in, up_weight, preferred_element_type=jnp.float32), approximate=True)
    lifted = lifted.astype(jnp.bfloat16)
    width_part = FF // N_TENSOR
    mlp_total = jnp.zeros((IMG * SEQ, D), jnp.float32)
    for block_index in range(N_TENSOR):
        low = block_index * width_part
        partial_value = jnp.dot(lifted[:, low:low + width_part], down_weight[low:low + width_part], preferred_element_type=jnp.float32)
        mlp_total = mlp_total + lax.optimization_barrier(partial_value.astype(jnp.bfloat16)).astype(jnp.float32)
    hidden = hidden + gate_mlp * mlp_total.reshape(IMG, SEQ, D)
    final_in = modulate(hidden, shift_out, scale_out).astype(jnp.bfloat16).reshape(IMG * SEQ, D)
    return jnp.dot(final_in, final_weight, preferred_element_type=jnp.float32).reshape(IMG, LAT)

def reference(noise_start, timesteps, class_labels, mixing, class_table, time_in, time_out, ada_weight, final_ada, patch_weight, q_weight, kv_weight, out_weight, up_weight, down_weight, final_weight):
    params = (class_table, time_in, time_out, ada_weight, final_ada, patch_weight, q_weight, kv_weight, out_weight, up_weight, down_weight, final_weight)
    alphas = alpha_at(timesteps)
    alpha_now = alphas[:WINDOW]
    alpha_next = alphas[1:]
    keep_coef = jnp.sqrt(alpha_next / alpha_now)
    noise_coef = jnp.sqrt(1.0 - alpha_next) - jnp.sqrt(alpha_next * (1.0 - alpha_now) / alpha_now)
    states = jnp.broadcast_to(noise_start[None], (WINDOW, IMG, LAT))
    previous = states
    residual_rows = []
    for iteration in range(ITERS):
        inputs = jnp.concatenate([noise_start[None], states[:WINDOW - 1]], axis=0)
        predicted = lax.map(lambda packed: denoise(packed[0], packed[1], packed[2], params), (inputs, timesteps[:WINDOW], class_labels))
        drifts = (keep_coef - 1.0)[:, None, None] * inputs + noise_coef[:, None, None] * predicted
        picard_map = noise_start[None] + jnp.cumsum(drifts, axis=0)
        residual_rows.append(lax.optimization_barrier(jnp.mean(jnp.square(picard_map - states), axis=(1, 2))))
        mixed_states = picard_map + mixing[iteration][:, None, None] * (picard_map - previous)
        previous = picard_map
        states = mixed_states
    return (states, jnp.stack(residual_rows))
```

```python
import math

import jax
import jax.numpy as jnp
import numpy as np
from jax import lax
from jax.experimental import pallas as pl
from jax.experimental.pallas import tpu as pltpu
from jax.sharding import Mesh
from jax.sharding import PartitionSpec as P

D = 768
HEADS = 12
SEQ = 1024
PATCH = 16
CLASSES = 1000
FREQ = 256
ITERS = 2
FF_OWN = 1536
TM = ("tm_0", "tm_1", "tm_2")
PLANE = ("tm_1", "tm_2")

norm_eps = 1e-06
plan_steps = 1000

OWN = SEQ // 2
LANES = 128
PER_ROW = LANES // PATCH
DENSE = OWN // PER_ROW
HALF = D // 2
ROWS = 256
GROUPS = ROWS // DENSE
MIB = 1 << 20
Q_FACTOR = math.log2(math.e) / math.sqrt(D // HEADS)


def log_table():
    levels = np.arange(plan_steps, dtype=np.float64)
    beta_values = 0.0001 + (0.02 - 0.0001) * levels / (plan_steps - 1)
    return np.cumsum(np.log(1.0 - beta_values)).astype(np.float32)


def angle_tables():
    rates = np.exp(-math.log(10000.0) * np.arange(HALF, dtype=np.float64) / HALF)
    coarse = (PER_ROW * np.arange(SEQ // PER_ROW, dtype=np.float64))[:, None] * rates[None, :]
    fine = np.arange(PER_ROW, dtype=np.float64)[:, None] * rates[None, :]
    coarse = np.concatenate([np.sin(coarse), np.cos(coarse)], axis=1)
    fine = np.concatenate([np.sin(fine), np.cos(fine)], axis=1)
    return coarse.astype(np.float32), fine.astype(np.float32)


def alpha_at(moments):
    matches = moments[:, None] == jnp.arange(plan_steps, dtype=jnp.int32)[None, :]
    return jnp.exp(jnp.sum(jnp.where(matches, jnp.asarray(log_table())[None, :], 0.0), axis=1))


def time_features(moment):
    half_count = FREQ // 2
    freq_rates = jnp.exp(
        -math.log(10000.0) * jnp.arange(half_count, dtype=jnp.float32) / half_count
    )
    angles = moment.astype(jnp.float32) * freq_rates
    return jnp.concatenate([jnp.cos(angles), jnp.sin(angles)])[None, :]


def pick_entry(vector, wanted):
    matches = jnp.arange(vector.shape[0], dtype=jnp.int32) == wanted
    return jnp.sum(jnp.where(matches, vector, 0))


def normed(values, shift, scale):
    center = values - jnp.mean(values, axis=-1, keepdims=True)
    spread = jnp.mean(center * center, axis=-1, keepdims=True)
    return center * lax.rsqrt(spread + norm_eps) * (1.0 + scale) + shift


def matmul(a, b):
    return jnp.dot(a, b, preferred_element_type=jnp.float32)


def attend_kernel(
    member_ref,
    tokens_ref,
    modul_ref,
    coarse_ref,
    fine_ref,
    patch_ref,
    q_hbm,
    kv_hbm,
    hidden_ref,
    attended_ref,
    q_w,
    kv_w,
    queries,
    keys,
    values,
    scores,
    sems,
):
    copy_q = pltpu.make_async_copy(q_hbm, q_w, sems.at[0])
    copy_kv = pltpu.make_async_copy(kv_hbm, kv_w, sems.at[1])
    copy_kv.start()
    copy_q.start()
    member = member_ref[0]
    shift = modul_ref[:, 0:D]
    scale = modul_ref[:, D : 2 * D]
    patch = patch_ref[...]
    dense_lane = lax.broadcasted_iota(jnp.int32, (DENSE, LANES), 1) // PATCH
    for pair in range(HEADS // 2):
        values[:, pair * 256 + LANES : (pair + 1) * 256] = jnp.ones((SEQ, LANES), jnp.bfloat16)

    def embedded(dense, coarse, first_group):
        coarse_sin, coarse_cos = coarse[:, :HALF], coarse[:, HALF:]
        pieces = []
        for group in range(first_group, first_group + GROUPS):
            picked = jnp.where(dense_lane == group, dense, jnp.zeros_like(dense))
            fine_sin = fine_ref[group : group + 1, 0:HALF]
            fine_cos = fine_ref[group : group + 1, HALF:D]
            places = jnp.concatenate(
                [
                    coarse_sin * fine_cos + coarse_cos * fine_sin,
                    coarse_cos * fine_cos - coarse_sin * fine_sin,
                ],
                axis=1,
            )
            pieces.append(matmul(picked, patch) + places)
        return jnp.concatenate(pieces, axis=0)

    waited = False
    for half in range(2):
        start = pl.multiple_of((member if half == 0 else 1 - member) * DENSE, DENSE)
        dense = tokens_ref[pl.ds(start, DENSE), :]
        coarse = coarse_ref[pl.ds(start, DENSE), :]
        for block in range(OWN // ROWS):
            low = block * ROWS
            hidden = embedded(dense, coarse, block * GROUPS)
            attn_in = normed(hidden, shift, scale).astype(jnp.bfloat16)
            if not waited:
                copy_kv.wait()
                copy_q.wait()
                waited = True
            if half == 0:
                hidden_ref[low : low + ROWS, :] = hidden
                queries[low : low + ROWS, :] = (matmul(attn_in, q_w[...]) * Q_FACTOR).astype(
                    jnp.bfloat16
                )
            both = matmul(attn_in, kv_w[...]).astype(jnp.bfloat16)
            at = half * OWN + low
            keys[at : at + ROWS, :] = both[:, :D]
            for pair in range(HEADS // 2):
                values[at : at + ROWS, pair * 256 : pair * 256 + LANES] = both[
                    :, D + pair * LANES : D + (pair + 1) * LANES
                ]

    lane = lax.broadcasted_iota(jnp.int32, (ROWS, LANES), 1)
    units = [
        (pair, block, odd)
        for pair in range(HEADS // 2)
        for block in range(OWN // ROWS)
        for odd in range(2)
    ]

    def score(unit, slot):
        pair, block, odd = unit
        q = queries[block * ROWS : (block + 1) * ROWS, pair * LANES : (pair + 1) * LANES]
        q = jnp.where((lane >= LANES // 2) == bool(odd), q, jnp.zeros_like(q))
        k = keys[:, pair * LANES : (pair + 1) * LANES]
        scores[slot] = lax.dot_general(
            q, k, (((1,), (1,)), ((), ())), preferred_element_type=jnp.float32
        )

    def weigh(unit, slot):
        pair, block, odd = unit
        s = scores[slot]
        e = jnp.exp2(s - jnp.max(s, axis=1, keepdims=True)).astype(jnp.bfloat16)
        o = matmul(e, values[:, pair * 256 : (pair + 1) * 256])
        return o[:, :LANES] / o[:, LANES:]

    score(units[0], 0)
    even = None
    for at, unit in enumerate(units):
        if at + 1 < len(units):
            score(units[at + 1], (at + 1) % 2)
        out = weigh(unit, at % 2)
        pair, block, odd = unit
        if odd:
            attended_ref[block * ROWS : (block + 1) * ROWS, pair * LANES : (pair + 1) * LANES] = (
                jnp.where(lane < LANES // 2, even, out).astype(jnp.bfloat16)
            )
        else:
            even = out


def attend(member, tokens, modul, coarse, fine, patch, q_weight, kv_weight):
    vmem = pl.BlockSpec(memory_space=pltpu.VMEM)
    hbm = pl.BlockSpec(memory_space=pl.ANY)
    return pl.pallas_call(
        attend_kernel,
        out_shape=(
            jax.ShapeDtypeStruct((OWN, D), jnp.float32),
            jax.ShapeDtypeStruct((OWN, D), jnp.bfloat16),
        ),
        in_specs=[pl.BlockSpec(memory_space=pltpu.SMEM)] + [vmem] * 5 + [hbm] * 2,
        out_specs=(vmem, vmem),
        scratch_shapes=[
            pltpu.VMEM((D, D), jnp.bfloat16),
            pltpu.VMEM((D, 2 * D), jnp.bfloat16),
            pltpu.VMEM((OWN, D), jnp.bfloat16),
            pltpu.VMEM((SEQ, D), jnp.bfloat16),
            pltpu.VMEM((SEQ, 2 * D), jnp.bfloat16),
            pltpu.VMEM((2, ROWS, SEQ), jnp.float32),
            pltpu.SemaphoreType.DMA((2,)),
        ],
        compiler_params=pltpu.CompilerParams(vmem_limit_bytes=32 * MIB),
        name="attend",
    )(member, tokens, modul, coarse, fine, patch, q_weight, kv_weight)


def finish_kernel(
    coef_ref,
    state_ref,
    modul_ref,
    final_mod_ref,
    hidden_ref,
    attended_ref,
    final_ref,
    out_hbm,
    up_a_hbm,
    down_a_hbm,
    up_b_hbm,
    down_b_hbm,
    drift_ref,
    out_w,
    up_w,
    down_w,
    sems,
):
    copies = [
        pltpu.make_async_copy(out_hbm, out_w, sems.at[0]),
        pltpu.make_async_copy(up_a_hbm, up_w.at[0], sems.at[1]),
        pltpu.make_async_copy(down_a_hbm, down_w.at[0], sems.at[2]),
        pltpu.make_async_copy(up_b_hbm, up_w.at[1], sems.at[3]),
        pltpu.make_async_copy(down_b_hbm, down_w.at[1], sems.at[4]),
    ]
    for copy in copies:
        copy.start()
    gate_attn, shift_mlp, scale_mlp, gate_mlp = [
        modul_ref[:, i * D : (i + 1) * D] for i in range(2, 6)
    ]
    shift_out, scale_out = final_mod_ref[:, 0:D], final_mod_ref[:, D : 2 * D]
    final_w = final_ref[...]
    dense_lane = lax.broadcasted_iota(jnp.int32, (DENSE, LANES), 1) // PATCH
    keep_less, noise_coef = coef_ref[0], coef_ref[1]
    eps = jnp.zeros((DENSE, LANES), jnp.float32)
    for block in range(OWN // ROWS):
        rows = slice(block * ROWS, (block + 1) * ROWS)
        if block == 0:
            copies[0].wait()
        h1 = hidden_ref[rows, :] + gate_attn * matmul(attended_ref[rows, :], out_w[...])
        mlp_in = normed(h1, shift_mlp, scale_mlp).astype(jnp.bfloat16)
        mlp_out = None
        for part in range(2):
            if block == 0:
                copies[1 + 2 * part].wait()
            lifted = jax.nn.gelu(matmul(mlp_in, up_w[part]), approximate=True).astype(jnp.bfloat16)
            if block == 0:
                copies[2 + 2 * part].wait()
            share = matmul(lifted, down_w[part]).astype(jnp.bfloat16).astype(jnp.float32)
            mlp_out = share if part == 0 else mlp_out + share
        h2 = h1 + gate_mlp * mlp_out
        final_in = normed(h2, shift_out, scale_out).astype(jnp.bfloat16)
        predicted = matmul(final_in, final_w)
        for group in range(GROUPS):
            eps = jnp.where(
                dense_lane == block * GROUPS + group,
                predicted[group * DENSE : (group + 1) * DENSE, :],
                eps,
            )
    drift_ref[...] = keep_less * state_ref[...] + noise_coef * eps


def finish(coefs, state, modul, final_mod, hidden, attended, final_w, out_w, own, other):
    vmem = pl.BlockSpec(memory_space=pltpu.VMEM)
    hbm = pl.BlockSpec(memory_space=pl.ANY)
    return pl.pallas_call(
        finish_kernel,
        out_shape=jax.ShapeDtypeStruct((DENSE, LANES), jnp.float32),
        in_specs=[pl.BlockSpec(memory_space=pltpu.SMEM)] + [vmem] * 6 + [hbm] * 5,
        out_specs=vmem,
        scratch_shapes=[
            pltpu.VMEM((D, D), jnp.bfloat16),
            pltpu.VMEM((2, D, FF_OWN), jnp.bfloat16),
            pltpu.VMEM((2, FF_OWN, D), jnp.bfloat16),
            pltpu.SemaphoreType.DMA((5,)),
        ],
        compiler_params=pltpu.CompilerParams(vmem_limit_bytes=32 * MIB),
        name="finish",
    )(coefs, state, modul, final_mod, hidden, attended, final_w, out_w, *own, *other)


def from_everyone(array, axis):
    copies = jnp.broadcast_to(array, (lax.axis_size(axis), *array.shape))
    return lax.all_to_all(copies, axis, split_axis=0, concat_axis=0, tiled=True)


def earlier_sum(pieces, here):
    before = jnp.zeros(pieces.shape[1:], jnp.float32)
    total = before
    for k in range(pieces.shape[0]):
        piece = pieces[k].astype(jnp.float32)
        before = before + jnp.where(k < here, piece, 0.0)
        total = total + piece
    return before, total


def entering(array):
    pieces = from_everyone(array.astype(jnp.bfloat16), PLANE)
    inside, total = earlier_sum(pieces, lax.axis_index(PLANE))
    planes = from_everyone(total.astype(jnp.bfloat16), "tm_0")
    outside, _ = earlier_sum(planes, lax.axis_index("tm_0"))
    return inside + outside


def condition(moment, label, class_table, time_in, time_out, ada_weight, final_ada):
    features = time_features(moment).astype(jnp.bfloat16)
    time_hidden = jax.nn.silu(matmul(features, time_in)).astype(jnp.bfloat16)
    time_embed = matmul(time_hidden, time_out)
    classes = lax.dynamic_slice_in_dim(class_table, label, 1, 0).astype(jnp.float32)
    summed = jax.nn.silu(time_embed + classes).astype(jnp.bfloat16)
    return matmul(summed, ada_weight), matmul(summed, final_ada)


def per_device(
    noise_start,
    timesteps,
    class_labels,
    mixing,
    class_table,
    time_in,
    time_out,
    ada_weight,
    final_ada,
    patch_weight,
    q_weight,
    kv_weight,
    out_weight,
    up_weight,
    down_weight,
    final_weight,
):
    swap = [(0, 1), (1, 0)]
    own = (up_weight, down_weight)
    other = (
        lax.ppermute(up_weight, "tensor", swap),
        lax.ppermute(down_weight, "tensor", swap),
    )
    count = lax.axis_size(TM)
    mixing_behind = lax.ppermute(mixing[0], TM, [(k, k + 1) for k in range(count - 1)])[0]
    window_point = lax.axis_index(TM)
    member = lax.axis_index("tensor").astype(jnp.int32)
    moment_now = pick_entry(timesteps, window_point)
    moment_next = pick_entry(timesteps, window_point + 1)
    alphas = alpha_at(jnp.stack([moment_now, moment_next]))
    keep_coef = jnp.sqrt(alphas[1] / alphas[0])
    noise_coef = jnp.sqrt(1.0 - alphas[1]) - jnp.sqrt(alphas[1] * (1.0 - alphas[0]) / alphas[0])
    coefs = jnp.stack([keep_coef - 1.0, noise_coef])
    modul, final_mod = condition(
        moment_now, class_labels[0, 0], class_table, time_in, time_out, ada_weight, final_ada
    )
    coarse, fine = (jnp.asarray(table) for table in angle_tables())
    patch_tiled = jnp.tile(patch_weight, (PER_ROW, 1))
    final_tiled = jnp.tile(final_weight, (1, PER_ROW))
    noise = noise_start.reshape(2 * DENSE, LANES)
    noise_own = lax.dynamic_slice_in_dim(noise, member * DENSE, DENSE, 0)
    member = member[None]

    def drift(tokens, state):
        hidden, attended = attend(
            member, tokens, modul, coarse, fine, patch_tiled, q_weight, kv_weight
        )
        return finish(
            coefs, state, modul, final_mod, hidden, attended, final_tiled, out_weight, own, other
        )

    drift_first = drift(noise.astype(jnp.bfloat16), noise_own)
    before = entering(drift_first)
    reached_first = before + drift_first
    state_in = noise_own + (1.0 + mixing_behind) * before
    tokens = lax.all_gather(state_in.astype(jnp.bfloat16), "tensor", tiled=True)
    drift_second = drift(tokens, state_in)
    reached = entering(drift_second) + drift_second
    moved = reached + mixing[1, 0] * (reached - reached_first)
    missed = reached - (1.0 + mixing[0, 0]) * reached_first
    lane = lax.broadcasted_iota(jnp.int32, (8, LANES), 1)
    sums = jnp.where(
        lane == 0, jnp.sum(jnp.square(reached_first)), jnp.where(lane == 1, jnp.sum(jnp.square(missed)), 0.0)
    )
    packed = lax.all_gather(jnp.concatenate([noise_own + moved, sums]), "tensor")
    states = packed[:, :DENSE].reshape(1, 1, 2 * DENSE * LANES)
    residuals = (packed[0, DENSE, :ITERS] + packed[1, DENSE, :ITERS]) / (2 * DENSE * LANES)
    return (states, residuals[:, None])


def solution(mesh):
    split = Mesh(
        mesh.devices.reshape(8, 4, 4, mesh.shape["tensor"]), ("tm_0", "tm_1", "tm_2", "tensor")
    )
    placed = (
        P(),
        P(),
        P(TM, None),
        P(None, TM),
        P(),
        P(),
        P(),
        P(),
        P(),
        P(),
        P(),
        P(),
        P(),
        P(None, "tensor"),
        P("tensor", None),
        P(),
    )
    return jax.shard_map(
        per_device,
        mesh=split,
        in_specs=placed,
        out_specs=(P(TM, None, None), P(None, TM)),
        check_vma=False,
    )
```

```python
import math

import jax
import jax.numpy as jnp
import numpy as np
from jax import lax
from jax.experimental import pallas as pl
from jax.experimental.pallas import tpu as pltpu
from jax.sharding import Mesh
from jax.sharding import PartitionSpec as P

D = 768
HEADS = 12
SEQ = 1024
PATCH = 16
FREQ = 256
ITERS = 2
FF_OWN = 1536
TM = ("tm_0", "tm_1", "tm_2")
PLANE = ("tm_1", "tm_2")

norm_eps = 1e-06
plan_steps = 1000

OWN = SEQ // 2
LANES = 128
PER_ROW = LANES // PATCH
DENSE = OWN // PER_ROW
HALF = D // 2
ROWS = 256
GROUPS = ROWS // DENSE
MIB = 1 << 20
EXTRA = 8
FULL = DENSE + EXTRA
STEP = 32
PAIRS = HEADS // 2
Q_FACTOR = math.log2(math.e) / math.sqrt(D // HEADS)


def log_table():
    levels = np.arange(plan_steps, dtype=np.float64)
    beta_values = 0.0001 + (0.02 - 0.0001) * levels / (plan_steps - 1)
    table = np.zeros((8, LANES), np.float32)
    table.reshape(-1)[:plan_steps] = np.cumsum(np.log(1.0 - beta_values))
    return table


def angle_table(width, steps, first):
    rates = np.exp(-math.log(10000.0) * np.arange(width, dtype=np.float64) / width)
    angles = np.asarray(steps, np.float64)[:, None] * rates[None, :]
    parts = [np.cos(angles), np.sin(angles)]
    if first == "sin":
        parts = parts[::-1]
    return np.concatenate(parts, axis=1).astype(np.float32)


def place_tables():
    coarse = angle_table(HALF, PER_ROW * np.arange(SEQ // PER_ROW), "sin")
    return coarse, angle_table(HALF, np.arange(PER_ROW), "sin")


def time_table():
    count = np.arange(STEP)
    return np.concatenate(
        [angle_table(FREQ // 2, STEP * count, "cos"), angle_table(FREQ // 2, count, "cos")]
    )


def normed(values, shift, scale):
    center = values - jnp.mean(values, axis=-1, keepdims=True)
    spread = jnp.mean(center * center, axis=-1, keepdims=True)
    return center * lax.rsqrt(spread + norm_eps) * (1.0 + scale) + shift


def matmul(a, b):
    return jnp.dot(a, b, preferred_element_type=jnp.float32)


VMEM = pl.BlockSpec(memory_space=pltpu.VMEM)
SMEM = pl.BlockSpec(memory_space=pltpu.SMEM)
HBM = pl.BlockSpec(memory_space=pltpu.HBM)


def condition_kernel(
    where_ref,
    timesteps_ref,
    label_ref,
    noise_ref,
    logs_hbm,
    table_hbm,
    class_hbm,
    time_in_hbm,
    time_out_hbm,
    ada_hbm,
    final_ada_hbm,
    modul_ref,
    coef_ref,
    tokens_ref,
    logs,
    table,
    class_rows,
    time_in,
    time_out,
    ada,
    sems,
):
    label = label_ref[0, 0]
    block = pl.multiple_of((label // 8) * 8, 8)
    copies = [
        pltpu.make_async_copy(table_hbm, table, sems.at[0]),
        pltpu.make_async_copy(time_in_hbm, time_in, sems.at[1]),
        pltpu.make_async_copy(time_out_hbm, time_out, sems.at[2]),
        pltpu.make_async_copy(class_hbm.at[pl.ds(block, 8), :], class_rows, sems.at[3]),
        pltpu.make_async_copy(logs_hbm, logs, sems.at[4]),
    ]
    for column in range(8):
        source = ada_hbm if column < 6 else final_ada_hbm
        at = column if column < 6 else column - 6
        copies.append(
            pltpu.make_async_copy(
                source.at[:, at * D : (at + 1) * D], ada.at[column], sems.at[5 + column]
            )
        )
    for copy in copies:
        copy.start()
    tokens_ref[...] = noise_ref[...].astype(jnp.bfloat16)
    point = where_ref[3]
    now, after = timesteps_ref[point], timesteps_ref[point + 1]

    copies[0].wait()
    high = table[pl.ds(now // STEP, 1), :]
    low = table[pl.ds(STEP + now % STEP, 1), :]
    half = FREQ // 2
    high_cos, high_sin, low_cos, low_sin = high[:, :half], high[:, half:], low[:, :half], low[:, half:]
    features = jnp.concatenate(
        [high_cos * low_cos - high_sin * low_sin, high_sin * low_cos + high_cos * low_sin], axis=1
    ).astype(jnp.bfloat16)
    copies[1].wait()
    time_hidden = jax.nn.silu(matmul(features, time_in[...])).astype(jnp.bfloat16)
    copies[2].wait()
    time_embed = matmul(time_hidden, time_out[...])
    copies[3].wait()
    row = lax.broadcasted_iota(jnp.int32, (8, D), 0)
    classes = jnp.sum(
        jnp.where(row == label % 8, class_rows[...].astype(jnp.float32), 0.0), axis=0, keepdims=True
    )
    summed = jax.nn.silu(time_embed + classes).astype(jnp.bfloat16)

    copies[4].wait()
    entry = lax.broadcasted_iota(jnp.int32, (8, LANES), 0) * LANES + lax.broadcasted_iota(
        jnp.int32, (8, LANES), 1
    )

    def alpha(moment):
        found = jnp.where(entry == moment, logs[...], 0.0)
        total = jnp.sum(jnp.sum(found, axis=1, keepdims=True), axis=0, keepdims=True)
        return jnp.exp(jnp.broadcast_to(total, (8, LANES)))

    alpha_now, alpha_after = alpha(now), alpha(after)
    keep = jnp.sqrt(alpha_after / alpha_now)
    coef = jnp.sqrt(1.0 - alpha_after) - jnp.sqrt(alpha_after * (1.0 - alpha_now) / alpha_now)
    coef_ref[0:8, :] = keep - 1.0
    coef_ref[8:16, :] = coef
    for column in range(8):
        copies[5 + column].wait()
        modul_ref[:, column * D : (column + 1) * D] = matmul(summed, ada[column])


def condition(where, timesteps, labels, noise, *weights):
    return pl.pallas_call(
        condition_kernel,
        out_shape=(
            jax.ShapeDtypeStruct((1, 8 * D), jnp.float32),
            jax.ShapeDtypeStruct((16, LANES), jnp.float32),
            jax.ShapeDtypeStruct((2 * DENSE, LANES), jnp.bfloat16),
        ),
        in_specs=[SMEM] * 3 + [VMEM] + [HBM] * 7,
        out_specs=(VMEM, VMEM, VMEM),
        scratch_shapes=[
            pltpu.VMEM((8, LANES), jnp.float32),
            pltpu.VMEM((2 * STEP, FREQ), jnp.float32),
            pltpu.VMEM((8, D), jnp.bfloat16),
            pltpu.VMEM((FREQ, D), jnp.bfloat16),
            pltpu.VMEM((D, D), jnp.bfloat16),
            pltpu.VMEM((8, D, D), jnp.bfloat16),
            pltpu.SemaphoreType.DMA((13,)),
        ],
        compiler_params=pltpu.CompilerParams(vmem_limit_bytes=24 * MIB),
        name="condition",
    )(where, timesteps, labels, noise, log_table(), time_table(), *weights)


def denoise_kernel(
    where_ref,
    mixing_ref,
    tokens_ref,
    state_ref,
    modul_ref,
    coef_ref,
    coarse_hbm,
    fine_hbm,
    patch_hbm,
    kv_hbm,
    q_hbm,
    out_hbm,
    final_hbm,
    up_a_hbm,
    down_a_hbm,
    up_b_hbm,
    down_b_hbm,
    drift_ref,
    payload_ref,
    coarse_w,
    fine_w,
    patch_w,
    kv_w,
    q_w,
    out_w,
    final_w,
    up_w,
    down_w,
    hidden_all,
    queries,
    keys,
    values,
    attended,
    scores,
    sems,
):
    sources = [coarse_hbm, fine_hbm, patch_hbm, kv_hbm, q_hbm, out_hbm, final_hbm]
    sources += [up_a_hbm, down_a_hbm, up_b_hbm, down_b_hbm]
    targets = [coarse_w, fine_w, patch_w, kv_w, q_w, out_w, final_w]
    targets += [up_w.at[0], down_w.at[0], up_w.at[1], down_w.at[1]]
    copies = [
        pltpu.make_async_copy(source, target, sems.at[at])
        for at, (source, target) in enumerate(zip(sources, targets))
    ]
    for copy in copies[:5]:
        copy.start()
    member = where_ref[0]
    mods = [modul_ref[:, i * D : (i + 1) * D] for i in range(8)]
    shift_attn, scale_attn, gate_attn, shift_mlp, scale_mlp, gate_mlp, shift_out, scale_out = mods
    dense_lane = lax.broadcasted_iota(jnp.int32, (DENSE, LANES), 1) // PATCH
    for pair in range(PAIRS):
        values[pair, :, LANES:] = jnp.ones((SEQ, LANES), jnp.bfloat16)
    for copy in copies[:3]:
        copy.wait()
    patch = jnp.concatenate([patch_w[...]] * PER_ROW, axis=0)

    def embedded(dense, coarse, first_group):
        coarse_sin, coarse_cos = coarse[:, :HALF], coarse[:, HALF:]
        pieces = []
        for group in range(first_group, first_group + GROUPS):
            picked = jnp.where(dense_lane == group, dense, jnp.zeros_like(dense))
            fine_sin = fine_w[group : group + 1, 0:HALF]
            fine_cos = fine_w[group : group + 1, HALF:D]
            places = jnp.concatenate(
                [
                    coarse_sin * fine_cos + coarse_cos * fine_sin,
                    coarse_cos * fine_cos - coarse_sin * fine_sin,
                ],
                axis=1,
            )
            pieces.append(matmul(picked, patch) + places)
        return jnp.concatenate(pieces, axis=0)

    for half in range(2):
        start = pl.multiple_of((member if half == 0 else 1 - member) * DENSE, DENSE)
        dense = tokens_ref[pl.ds(start, DENSE), :]
        coarse = coarse_w[pl.ds(start, DENSE), :]
        for block in range(OWN // ROWS):
            low = block * ROWS
            hidden = embedded(dense, coarse, block * GROUPS)
            attn_in = normed(hidden, shift_attn, scale_attn).astype(jnp.bfloat16)
            if half == 0 and block == 0:
                copies[3].wait()
                copies[4].wait()
                for copy in copies[5:]:
                    copy.start()
            if half == 0:
                hidden_all[low : low + ROWS, :] = hidden
                q = (matmul(attn_in, q_w[...]) * Q_FACTOR).astype(jnp.bfloat16)
                for pair in range(PAIRS):
                    queries[pair, low : low + ROWS, :] = q[:, pair * LANES : (pair + 1) * LANES]
            both = matmul(attn_in, kv_w[...]).astype(jnp.bfloat16)
            at = half * OWN + low
            for pair in range(PAIRS):
                here = pair * LANES
                keys[pair, at : at + ROWS, :] = both[:, here : here + LANES]
                values[pair, at : at + ROWS, 0:LANES] = both[:, D + here : D + here + LANES]

    lane = lax.broadcasted_iota(jnp.int32, (ROWS, LANES), 1)

    def score(pair, block, odd, slot):
        q = queries[pair, block * ROWS : (block + 1) * ROWS, :]
        q = jnp.where((lane >= LANES // 2) == bool(odd), q, jnp.zeros_like(q))
        scores[slot] = lax.dot_general(
            q, keys[pair], (((1,), (1,)), ((), ())), preferred_element_type=jnp.float32
        )

    def weigh(pair, slot):
        s = scores[slot]
        e = jnp.exp2(s - jnp.max(s, axis=1, keepdims=True)).astype(jnp.bfloat16)
        o = matmul(e, values[pair])
        return o[:, :LANES] / o[:, LANES:]

    def over_pair(pair, carry):
        score(pair, 0, 1, 1)
        outs = [weigh(pair, 0)]
        score(pair, 1, 0, 0)
        outs.append(weigh(pair, 1))
        score(pair, 1, 1, 1)
        outs.append(weigh(pair, 0))
        score(jnp.minimum(pair + 1, PAIRS - 1), 0, 0, 0)
        outs.append(weigh(pair, 1))
        at = pl.multiple_of(pair * LANES, LANES)
        for block in range(OWN // ROWS):
            attended[block * ROWS : (block + 1) * ROWS, pl.ds(at, LANES)] = jnp.where(
                lane < LANES // 2, outs[2 * block], outs[2 * block + 1]
            ).astype(jnp.bfloat16)
        return carry

    score(0, 0, 0, 0)
    lax.fori_loop(0, PAIRS, over_pair, 0)

    eps = jnp.zeros((DENSE, LANES), jnp.float32)
    chosen = (
        lax.broadcasted_iota(jnp.int32, (PATCH, LANES), 1) % PATCH
        == lax.broadcasted_iota(jnp.int32, (PATCH, LANES), 0)
    ).astype(jnp.bfloat16)
    copies[5].wait()
    copies[6].wait()
    final_tiled = matmul(final_w[...], chosen).astype(jnp.bfloat16)
    for block in range(OWN // ROWS):
        rows = slice(block * ROWS, (block + 1) * ROWS)
        h1 = hidden_all[rows, :] + gate_attn * matmul(attended[rows, :], out_w[...])
        mlp_in = normed(h1, shift_mlp, scale_mlp).astype(jnp.bfloat16)
        mlp_out = None
        for part in range(2):
            if block == 0:
                copies[7 + 2 * part].wait()
            lifted = jax.nn.gelu(matmul(mlp_in, up_w[part]), approximate=True).astype(jnp.bfloat16)
            if block == 0:
                copies[8 + 2 * part].wait()
            share = matmul(lifted, down_w[part]).astype(jnp.bfloat16).astype(jnp.float32)
            mlp_out = share if part == 0 else mlp_out + share
        h2 = h1 + gate_mlp * mlp_out
        final_in = normed(h2, shift_out, scale_out).astype(jnp.bfloat16)
        predicted = matmul(final_in, final_tiled)
        for group in range(GROUPS):
            eps = jnp.where(
                dense_lane == block * GROUPS + group,
                predicted[group * DENSE : (group + 1) * DENSE, :],
                eps,
            )
    drift = coef_ref[0:1, :] * state_ref[...] + coef_ref[8:9, :] * eps
    drift_ref[...] = drift
    mixing = jnp.full((EXTRA, LANES), mixing_ref[0, 0], jnp.float32)
    rounded = mixing.astype(jnp.bfloat16).astype(jnp.float32)
    row = lax.broadcasted_iota(jnp.int32, (EXTRA, LANES), 0)
    beside = jnp.where(row == 0, rounded, jnp.where(row == 1, mixing - rounded, 0.0))
    sent = jnp.concatenate([drift, beside], axis=0).astype(jnp.bfloat16)
    for copy in range(payload_ref.shape[0]):
        payload_ref[copy] = sent


def denoise(copies, where, mixing, tokens, state, modul, coefs, *weights):
    bf16 = jnp.bfloat16
    return pl.pallas_call(
        denoise_kernel,
        out_shape=(
            jax.ShapeDtypeStruct((DENSE, LANES), jnp.float32),
            jax.ShapeDtypeStruct((copies, FULL, LANES), bf16),
        ),
        in_specs=[SMEM] * 2 + [VMEM] * 4 + [HBM] * 11,
        out_specs=(VMEM, VMEM),
        scratch_shapes=[
            pltpu.VMEM((SEQ // PER_ROW, D), jnp.float32),
            pltpu.VMEM((PER_ROW, D), jnp.float32),
            pltpu.VMEM((PATCH, D), bf16),
            pltpu.VMEM((D, 2 * D), bf16),
            pltpu.VMEM((D, D), bf16),
            pltpu.VMEM((D, D), bf16),
            pltpu.VMEM((D, PATCH), bf16),
            pltpu.VMEM((2, D, FF_OWN), bf16),
            pltpu.VMEM((2, FF_OWN, D), bf16),
            pltpu.VMEM((OWN, D), jnp.float32),
            pltpu.VMEM((PAIRS, OWN, LANES), bf16),
            pltpu.VMEM((PAIRS, SEQ, LANES), bf16),
            pltpu.VMEM((PAIRS, SEQ, 2 * LANES), bf16),
            pltpu.VMEM((OWN, D), bf16),
            pltpu.VMEM((2, ROWS, SEQ), jnp.float32),
            pltpu.SemaphoreType.DMA((11,)),
        ],
        compiler_params=pltpu.CompilerParams(vmem_limit_bytes=48 * MIB),
        name="denoise",
    )(where, mixing, tokens, state, modul, coefs, *weights)


def plane_kernel(where_ref, pieces_ref, inside_ref, payload_ref):
    here = where_ref[1]
    count = pieces_ref.shape[0]
    before = jnp.zeros((DENSE, LANES), jnp.float32)
    total = before
    beside = jnp.zeros((EXTRA, LANES), jnp.float32)
    for k in range(count):
        piece = pieces_ref[k].astype(jnp.float32)
        before = before + jnp.where(k < here, piece[:DENSE], 0.0)
        total = total + piece[:DENSE]
        beside = jnp.where(k == here - 1, piece[DENSE:], beside)
    inside_ref[0:DENSE, :] = before
    inside_ref[DENSE:FULL, :] = beside
    last = pieces_ref[count - 1, DENSE:FULL, :].astype(jnp.float32)
    sent = jnp.concatenate([total, last], axis=0).astype(jnp.bfloat16)
    for copy in range(payload_ref.shape[0]):
        payload_ref[copy] = sent


def plane(where, pieces, planes):
    return pl.pallas_call(
        plane_kernel,
        out_shape=(
            jax.ShapeDtypeStruct((FULL, LANES), jnp.float32),
            jax.ShapeDtypeStruct((planes, FULL, LANES), jnp.bfloat16),
        ),
        in_specs=[SMEM, VMEM],
        out_specs=(VMEM, VMEM),
        compiler_params=pltpu.CompilerParams(vmem_limit_bytes=8 * MIB),
        name="plane",
    )(where, pieces)


def entered(where_ref, planes_ref, inside_ref):
    before = inside_ref[0:DENSE, :]
    for k in range(planes_ref.shape[0]):
        piece = planes_ref[k, 0:DENSE, :].astype(jnp.float32)
        before = before + jnp.where(k < where_ref[2], piece, 0.0)
    return before


def advance_kernel(
    where_ref, planes_ref, inside_ref, drift_ref, noise_ref, reached_ref, state_ref, tokens_ref
):
    before = entered(where_ref, planes_ref, inside_ref)
    reached_ref[...] = before + drift_ref[...]
    beside = inside_ref[DENSE:FULL, :]
    for k in range(planes_ref.shape[0]):
        found = jnp.logical_and(where_ref[1] == 0, k == where_ref[2] - 1)
        beside = jnp.where(found, planes_ref[k, DENSE:FULL, :].astype(jnp.float32), beside)
    mixing = jnp.sum(beside, axis=0, keepdims=True)
    start = pl.multiple_of(where_ref[0] * DENSE, DENSE)
    state = noise_ref[pl.ds(start, DENSE), :] + (1.0 + mixing) * before
    state_ref[...] = state
    tokens_ref[...] = state.astype(jnp.bfloat16)


def advance(where, planes, inside, drift, noise):
    field = jax.ShapeDtypeStruct((DENSE, LANES), jnp.float32)
    return pl.pallas_call(
        advance_kernel,
        out_shape=(field, field, jax.ShapeDtypeStruct((DENSE, LANES), jnp.bfloat16)),
        in_specs=[SMEM] + [VMEM] * 4,
        out_specs=(VMEM, VMEM, VMEM),
        compiler_params=pltpu.CompilerParams(vmem_limit_bytes=8 * MIB),
        name="advance",
    )(where, planes, inside, drift, noise)


def close_kernel(
    where_ref, mixing_ref, planes_ref, inside_ref, drift_ref, noise_ref, first_ref, packed_ref
):
    reached = entered(where_ref, planes_ref, inside_ref) + drift_ref[...]
    first = first_ref[...]
    start = pl.multiple_of(where_ref[0] * DENSE, DENSE)
    packed_ref[0:DENSE, :] = (
        noise_ref[pl.ds(start, DENSE), :] + reached + mixing_ref[1, 0] * (reached - first)
    )
    missed = reached - (1.0 + mixing_ref[0, 0]) * first

    def total(values):
        return jnp.sum(jnp.sum(values * values, axis=1, keepdims=True), axis=0, keepdims=True)

    row = lax.broadcasted_iota(jnp.int32, (EXTRA, LANES), 0)
    packed_ref[DENSE:FULL, :] = jnp.where(row == 0, total(first), total(missed)) / (
        2 * DENSE * LANES
    )


def close(where, mixing, planes, inside, drift, noise, first):
    return pl.pallas_call(
        close_kernel,
        out_shape=jax.ShapeDtypeStruct((FULL, LANES), jnp.float32),
        in_specs=[SMEM] * 2 + [VMEM] * 5,
        out_specs=VMEM,
        compiler_params=pltpu.CompilerParams(vmem_limit_bytes=8 * MIB),
        name="close",
    )(where, mixing, planes, inside, drift, noise, first)


def exchanged(copies, axis):
    return lax.all_to_all(copies, axis, split_axis=0, concat_axis=0, tiled=True)


def per_device(
    noise_start,
    timesteps,
    class_labels,
    mixing,
    class_table,
    time_in,
    time_out,
    ada_weight,
    final_ada,
    patch_weight,
    q_weight,
    kv_weight,
    out_weight,
    up_weight,
    down_weight,
    final_weight,
):
    swap = [(0, 1), (1, 0)]
    up_other = lax.ppermute(up_weight, "tensor", swap)
    down_other = lax.ppermute(down_weight, "tensor", swap)
    where = jnp.stack(
        [lax.axis_index(axis) for axis in ("tensor", PLANE, "tm_0", TM)]
    ).astype(jnp.int32)
    noise = noise_start.reshape(2 * DENSE, LANES)
    modul, coefs, tokens = condition(
        where,
        timesteps,
        class_labels,
        noise,
        class_table,
        time_in,
        time_out,
        ada_weight,
        final_ada,
    )
    coarse, fine = place_tables()
    weights = (coarse, fine, patch_weight, kv_weight, q_weight, out_weight, final_weight)
    weights += (up_weight, down_weight, up_other, down_other)

    def scanned(tokens, state):
        drift, payload = denoise(
            lax.axis_size(PLANE), where, mixing, tokens, state, modul, coefs, *weights
        )
        pieces = exchanged(payload, PLANE)
        inside, payload = plane(where, pieces, lax.axis_size("tm_0"))
        return drift, inside, exchanged(payload, "tm_0")

    noise_own = lax.dynamic_slice_in_dim(noise, where[0] * DENSE, DENSE, 0)
    drift, inside, planes = scanned(tokens, noise_own)
    reached, state, tokens = advance(where, planes, inside, drift, noise)
    tokens = lax.all_gather(tokens, "tensor", tiled=True)
    drift, inside, planes = scanned(tokens, state)
    packed = lax.all_gather(
        close(where, mixing, planes, inside, drift, noise, reached), "tensor"
    )
    states = packed[:, :DENSE].reshape(1, 1, 2 * DENSE * LANES)
    residuals = packed[0, DENSE : DENSE + ITERS, :1] + packed[1, DENSE : DENSE + ITERS, :1]
    return (states, residuals)


def solution(mesh):
    split = Mesh(
        mesh.devices.reshape(8, 4, 4, mesh.shape["tensor"]), ("tm_0", "tm_1", "tm_2", "tensor")
    )
    placed = (
        P(),
        P(),
        P(TM, None),
        P(None, TM),
        P(),
        P(),
        P(),
        P(),
        P(),
        P(),
        P(),
        P(),
        P(),
        P(None, "tensor"),
        P("tensor", None),
        P(),
    )
    return jax.shard_map(
        per_device,
        mesh=split,
        in_specs=placed,
        out_specs=(P(TM, None, None), P(None, TM)),
        check_vma=False,
    )
```

```python
import math

import jax
import jax.numpy as jnp
import numpy as np
from jax import lax
from jax.experimental import pallas as pl
from jax.experimental.pallas import tpu as pltpu
from jax.sharding import Mesh
from jax.sharding import PartitionSpec as P

D = 768
HEADS = 12
SEQ = 1024
PATCH = 16
FREQ = 256
ITERS = 2
FF_OWN = 1536
TM = ("tm_0", "tm_1", "tm_2")
PLANE = ("tm_1", "tm_2")

norm_eps = 1e-06
plan_steps = 1000

OWN = SEQ // 2
LANES = 128
PER_ROW = LANES // PATCH
DENSE = OWN // PER_ROW
HALF = D // 2
ROWS = 256
GROUPS = ROWS // DENSE
MLP_ROWS = 512
MLP_CHUNK = 768
MIB = 1 << 20
EXTRA = 8
FULL = DENSE + EXTRA
STEP = 32
PAIRS = HEADS // 2
Q_FACTOR = math.log2(math.e) / math.sqrt(D // HEADS)


def log_table():
    levels = np.arange(plan_steps, dtype=np.float64)
    beta_values = 0.0001 + (0.02 - 0.0001) * levels / (plan_steps - 1)
    table = np.zeros((8, LANES), np.float32)
    table.reshape(-1)[:plan_steps] = np.cumsum(np.log(1.0 - beta_values))
    return table


def angle_table(width, steps, first):
    rates = np.exp(-math.log(10000.0) * np.arange(width, dtype=np.float64) / width)
    angles = np.asarray(steps, np.float64)[:, None] * rates[None, :]
    parts = [np.cos(angles), np.sin(angles)]
    if first == "sin":
        parts = parts[::-1]
    return np.concatenate(parts, axis=1).astype(np.float32)


def place_tables():
    coarse = angle_table(HALF, PER_ROW * np.arange(SEQ // PER_ROW), "sin")
    return coarse, angle_table(HALF, np.arange(PER_ROW), "sin")


def time_table():
    count = np.arange(STEP)
    return np.concatenate(
        [angle_table(FREQ // 2, STEP * count, "cos"), angle_table(FREQ // 2, count, "cos")]
    )


def normed(values, shift, scale):
    center = values - jnp.mean(values, axis=-1, keepdims=True)
    spread = jnp.mean(center * center, axis=-1, keepdims=True)
    return center * lax.rsqrt(spread + norm_eps) * (1.0 + scale) + shift


def matmul(a, b):
    return jnp.dot(a, b, preferred_element_type=jnp.float32)


VMEM = pl.BlockSpec(memory_space=pltpu.VMEM)
SMEM = pl.BlockSpec(memory_space=pltpu.SMEM)
HBM = pl.BlockSpec(memory_space=pltpu.HBM)


def condition_kernel(
    where_ref,
    timesteps_ref,
    label_ref,
    noise_ref,
    logs_hbm,
    table_hbm,
    class_hbm,
    time_in_hbm,
    time_out_hbm,
    ada_hbm,
    final_ada_hbm,
    modul_ref,
    coef_ref,
    tokens_ref,
    logs,
    table,
    class_rows,
    time_in,
    time_out,
    ada,
    sems,
):
    label = label_ref[0, 0]
    block = pl.multiple_of((label // 8) * 8, 8)
    copies = [
        pltpu.make_async_copy(table_hbm, table, sems.at[0]),
        pltpu.make_async_copy(time_in_hbm, time_in, sems.at[1]),
        pltpu.make_async_copy(time_out_hbm, time_out, sems.at[2]),
        pltpu.make_async_copy(class_hbm.at[pl.ds(block, 8), :], class_rows, sems.at[3]),
        pltpu.make_async_copy(logs_hbm, logs, sems.at[4]),
    ]
    for column in range(8):
        source = ada_hbm if column < 6 else final_ada_hbm
        at = column if column < 6 else column - 6
        copies.append(
            pltpu.make_async_copy(
                source.at[:, at * D : (at + 1) * D], ada.at[column], sems.at[5 + column]
            )
        )
    for copy in copies:
        copy.start()
    tokens_ref[...] = noise_ref[...].astype(jnp.bfloat16)
    point = where_ref[3]
    now, after = timesteps_ref[point], timesteps_ref[point + 1]

    copies[0].wait()
    high = table[pl.ds(now // STEP, 1), :]
    low = table[pl.ds(STEP + now % STEP, 1), :]
    half = FREQ // 2
    high_cos, high_sin, low_cos, low_sin = high[:, :half], high[:, half:], low[:, :half], low[:, half:]
    features = jnp.concatenate(
        [high_cos * low_cos - high_sin * low_sin, high_sin * low_cos + high_cos * low_sin], axis=1
    ).astype(jnp.bfloat16)
    copies[1].wait()
    time_hidden = jax.nn.silu(matmul(features, time_in[...])).astype(jnp.bfloat16)
    copies[2].wait()
    time_embed = matmul(time_hidden, time_out[...])
    copies[3].wait()
    row = lax.broadcasted_iota(jnp.int32, (8, D), 0)
    classes = jnp.sum(
        jnp.where(row == label % 8, class_rows[...].astype(jnp.float32), 0.0), axis=0, keepdims=True
    )
    summed = jax.nn.silu(time_embed + classes).astype(jnp.bfloat16)

    copies[4].wait()
    entry = lax.broadcasted_iota(jnp.int32, (8, LANES), 0) * LANES + lax.broadcasted_iota(
        jnp.int32, (8, LANES), 1
    )

    def alpha(moment):
        found = jnp.where(entry == moment, logs[...], 0.0)
        total = jnp.sum(jnp.sum(found, axis=1, keepdims=True), axis=0, keepdims=True)
        return jnp.exp(jnp.broadcast_to(total, (8, LANES)))

    alpha_now, alpha_after = alpha(now), alpha(after)
    keep = jnp.sqrt(alpha_after / alpha_now)
    coef = jnp.sqrt(1.0 - alpha_after) - jnp.sqrt(alpha_after * (1.0 - alpha_now) / alpha_now)
    coef_ref[0:8, :] = keep - 1.0
    coef_ref[8:16, :] = coef
    for column in range(8):
        copies[5 + column].wait()
        modul_ref[:, column * D : (column + 1) * D] = matmul(summed, ada[column])


def condition(where, timesteps, labels, noise, *weights):
    return pl.pallas_call(
        condition_kernel,
        out_shape=(
            jax.ShapeDtypeStruct((1, 8 * D), jnp.float32),
            jax.ShapeDtypeStruct((16, LANES), jnp.float32),
            jax.ShapeDtypeStruct((2 * DENSE, LANES), jnp.bfloat16),
        ),
        in_specs=[SMEM] * 3 + [VMEM] + [HBM] * 7,
        out_specs=(VMEM, VMEM, VMEM),
        scratch_shapes=[
            pltpu.VMEM((8, LANES), jnp.float32),
            pltpu.VMEM((2 * STEP, FREQ), jnp.float32),
            pltpu.VMEM((8, D), jnp.bfloat16),
            pltpu.VMEM((FREQ, D), jnp.bfloat16),
            pltpu.VMEM((D, D), jnp.bfloat16),
            pltpu.VMEM((8, D, D), jnp.bfloat16),
            pltpu.SemaphoreType.DMA((13,)),
        ],
        compiler_params=pltpu.CompilerParams(vmem_limit_bytes=62 * MIB),
        name="condition",
    )(where, timesteps, labels, noise, log_table(), time_table(), *weights)


def denoise_kernel(
    where_ref,
    mixing_ref,
    tokens_ref,
    state_ref,
    modul_ref,
    coef_ref,
    coarse_hbm,
    fine_hbm,
    patch_hbm,
    kv_hbm,
    q_hbm,
    out_hbm,
    final_hbm,
    up_a_hbm,
    down_a_hbm,
    up_b_hbm,
    down_b_hbm,
    drift_ref,
    payload_ref,
    coarse_w,
    fine_w,
    patch_w,
    kv_w,
    q_w,
    out_w,
    final_w,
    up_w,
    down_w,
    hidden_all,
    queries,
    keys,
    values,
    attended,
    scores,
    sems,
):
    sources = [coarse_hbm, fine_hbm, patch_hbm, kv_hbm, q_hbm, out_hbm, final_hbm]
    sources += [up_a_hbm, down_a_hbm, up_b_hbm, down_b_hbm]
    targets = [coarse_w, fine_w, patch_w, kv_w, q_w, out_w, final_w]
    targets += [up_w.at[0], down_w.at[0], up_w.at[1], down_w.at[1]]
    copies = [
        pltpu.make_async_copy(source, target, sems.at[at])
        for at, (source, target) in enumerate(zip(sources, targets))
    ]
    for copy in copies[:5]:
        copy.start()
    member = where_ref[0]
    mods = [modul_ref[:, i * D : (i + 1) * D] for i in range(8)]
    shift_attn, scale_attn, gate_attn, shift_mlp, scale_mlp, gate_mlp, shift_out, scale_out = mods
    dense_lane = lax.broadcasted_iota(jnp.int32, (DENSE, LANES), 1) // PATCH
    for pair in range(PAIRS):
        values[pair, :, LANES:] = jnp.ones((SEQ, LANES), jnp.bfloat16)
    for copy in copies[:3]:
        copy.wait()
    patch = jnp.concatenate([patch_w[...]] * PER_ROW, axis=0)

    def embedded(dense, coarse, first_group):
        coarse_sin, coarse_cos = coarse[:, :HALF], coarse[:, HALF:]
        pieces = []
        for group in range(first_group, first_group + GROUPS):
            picked = jnp.where(dense_lane == group, dense, jnp.zeros_like(dense))
            fine_sin = fine_w[group : group + 1, 0:HALF]
            fine_cos = fine_w[group : group + 1, HALF:D]
            places = jnp.concatenate(
                [
                    coarse_sin * fine_cos + coarse_cos * fine_sin,
                    coarse_cos * fine_cos - coarse_sin * fine_sin,
                ],
                axis=1,
            )
            pieces.append(matmul(picked, patch) + places)
        return jnp.concatenate(pieces, axis=0)

    for half in range(2):
        start = pl.multiple_of((member if half == 0 else 1 - member) * DENSE, DENSE)
        dense = tokens_ref[pl.ds(start, DENSE), :]
        coarse = coarse_w[pl.ds(start, DENSE), :]
        for block in range(OWN // ROWS):
            low = block * ROWS
            hidden = embedded(dense, coarse, block * GROUPS)
            attn_in = normed(hidden, shift_attn, scale_attn).astype(jnp.bfloat16)
            if half == 0 and block == 0:
                copies[3].wait()
                copies[4].wait()
                for copy in copies[5:]:
                    copy.start()
            if half == 0:
                hidden_all[low : low + ROWS, :] = hidden
                q = (matmul(attn_in, q_w[...]) * Q_FACTOR).astype(jnp.bfloat16)
                for pair in range(PAIRS):
                    queries[pair, low : low + ROWS, :] = q[:, pair * LANES : (pair + 1) * LANES]
            both = matmul(attn_in, kv_w[...]).astype(jnp.bfloat16)
            at = half * OWN + low
            for pair in range(PAIRS):
                here = pair * LANES
                keys[pair, at : at + ROWS, :] = both[:, here : here + LANES]
                values[pair, at : at + ROWS, 0:LANES] = both[:, D + here : D + here + LANES]

    lane = lax.broadcasted_iota(jnp.int32, (ROWS, LANES), 1)

    def score(pair, block, odd, slot):
        q = queries[pair, block * ROWS : (block + 1) * ROWS, :]
        q = jnp.where((lane >= LANES // 2) == bool(odd), q, jnp.zeros_like(q))
        scores[slot] = lax.dot_general(
            q, keys[pair], (((1,), (1,)), ((), ())), preferred_element_type=jnp.float32
        )

    def weigh(pair, slot):
        s = scores[slot]
        e = jnp.exp2(s - jnp.max(s, axis=1, keepdims=True)).astype(jnp.bfloat16)
        o = matmul(e, values[pair])
        return o[:, :LANES] / o[:, LANES:]

    def over_pair(pair, carry):
        score(pair, 0, 1, 1)
        outs = [weigh(pair, 0)]
        score(pair, 1, 0, 0)
        outs.append(weigh(pair, 1))
        score(pair, 1, 1, 1)
        outs.append(weigh(pair, 0))
        score(jnp.minimum(pair + 1, PAIRS - 1), 0, 0, 0)
        outs.append(weigh(pair, 1))
        at = pl.multiple_of(pair * LANES, LANES)
        for block in range(OWN // ROWS):
            attended[block * ROWS : (block + 1) * ROWS, pl.ds(at, LANES)] = jnp.where(
                lane < LANES // 2, outs[2 * block], outs[2 * block + 1]
            ).astype(jnp.bfloat16)
        return carry

    score(0, 0, 0, 0)
    lax.fori_loop(0, PAIRS, over_pair, 0)

    eps = jnp.zeros((DENSE, LANES), jnp.float32)
    chosen = (
        lax.broadcasted_iota(jnp.int32, (PATCH, LANES), 1) % PATCH
        == lax.broadcasted_iota(jnp.int32, (PATCH, LANES), 0)
    ).astype(jnp.bfloat16)
    copies[5].wait()
    copies[6].wait()
    final_tiled = matmul(final_w[...], chosen).astype(jnp.bfloat16)
    for copy in copies[7:]:
        copy.wait()
    for block in range(OWN // MLP_ROWS):
        rows = slice(block * MLP_ROWS, (block + 1) * MLP_ROWS)
        h1 = hidden_all[rows, :] + gate_attn * matmul(attended[rows, :], out_w[...])
        mlp_in = normed(h1, shift_mlp, scale_mlp).astype(jnp.bfloat16)
        mlp_out = None
        steps = [(part, at) for part in range(2) for at in range(0, FF_OWN, MLP_CHUNK)]

        def raised(step):
            return matmul(mlp_in, up_w[step[0], :, step[1] : step[1] + MLP_CHUNK])

        ahead = raised(steps[0])
        shares = [None, None]
        for index, (part, at) in enumerate(steps):
            now = ahead
            if index + 1 < len(steps):
                ahead = raised(steps[index + 1])
            lifted = jax.nn.gelu(now, approximate=True).astype(jnp.bfloat16)
            product = matmul(lifted, down_w[part, at : at + MLP_CHUNK, :])
            shares[part] = product if shares[part] is None else shares[part] + product
        mlp_out = sum(share.astype(jnp.bfloat16).astype(jnp.float32) for share in shares)
        h2 = h1 + gate_mlp * mlp_out
        final_in = normed(h2, shift_out, scale_out).astype(jnp.bfloat16)
        predicted = matmul(final_in, final_tiled)
        for group in range(MLP_ROWS // DENSE):
            eps = jnp.where(
                dense_lane == block * (MLP_ROWS // DENSE) + group,
                predicted[group * DENSE : (group + 1) * DENSE, :],
                eps,
            )
    drift = coef_ref[0:1, :] * state_ref[...] + coef_ref[8:9, :] * eps
    drift_ref[...] = drift
    mixing = jnp.full((EXTRA, LANES), mixing_ref[0, 0], jnp.float32)
    rounded = mixing.astype(jnp.bfloat16).astype(jnp.float32)
    row = lax.broadcasted_iota(jnp.int32, (EXTRA, LANES), 0)
    beside = jnp.where(row == 0, rounded, jnp.where(row == 1, mixing - rounded, 0.0))
    sent = jnp.concatenate([drift, beside], axis=0).astype(jnp.bfloat16)
    for copy in range(payload_ref.shape[0]):
        payload_ref[copy] = sent


def denoise(copies, where, mixing, tokens, state, modul, coefs, *weights):
    bf16 = jnp.bfloat16
    return pl.pallas_call(
        denoise_kernel,
        out_shape=(
            jax.ShapeDtypeStruct((DENSE, LANES), jnp.float32),
            jax.ShapeDtypeStruct((copies, FULL, LANES), bf16),
        ),
        in_specs=[SMEM] * 2 + [VMEM] * 4 + [HBM] * 11,
        out_specs=(VMEM, VMEM),
        scratch_shapes=[
            pltpu.VMEM((SEQ // PER_ROW, D), jnp.float32),
            pltpu.VMEM((PER_ROW, D), jnp.float32),
            pltpu.VMEM((PATCH, D), bf16),
            pltpu.VMEM((D, 2 * D), bf16),
            pltpu.VMEM((D, D), bf16),
            pltpu.VMEM((D, D), bf16),
            pltpu.VMEM((D, PATCH), bf16),
            pltpu.VMEM((2, D, FF_OWN), bf16),
            pltpu.VMEM((2, FF_OWN, D), bf16),
            pltpu.VMEM((OWN, D), jnp.float32),
            pltpu.VMEM((PAIRS, OWN, LANES), bf16),
            pltpu.VMEM((PAIRS, SEQ, LANES), bf16),
            pltpu.VMEM((PAIRS, SEQ, 2 * LANES), bf16),
            pltpu.VMEM((OWN, D), bf16),
            pltpu.VMEM((2, ROWS, SEQ), jnp.float32),
            pltpu.SemaphoreType.DMA((11,)),
        ],
        compiler_params=pltpu.CompilerParams(vmem_limit_bytes=61 * MIB),
        name="denoise",
    )(where, mixing, tokens, state, modul, coefs, *weights)


def plane_kernel(where_ref, pieces_ref, inside_ref, payload_ref):
    here = where_ref[1]
    count = pieces_ref.shape[0]
    before = jnp.zeros((DENSE, LANES), jnp.float32)
    total = before
    beside = jnp.zeros((EXTRA, LANES), jnp.float32)
    for k in range(count):
        piece = pieces_ref[k].astype(jnp.float32)
        before = before + jnp.where(k < here, piece[:DENSE], 0.0)
        total = total + piece[:DENSE]
        beside = jnp.where(k == here - 1, piece[DENSE:], beside)
    inside_ref[0:DENSE, :] = before
    inside_ref[DENSE:FULL, :] = beside
    last = pieces_ref[count - 1, DENSE:FULL, :].astype(jnp.float32)
    sent = jnp.concatenate([total, last], axis=0).astype(jnp.bfloat16)
    for copy in range(payload_ref.shape[0]):
        payload_ref[copy] = sent


def plane(where, pieces, planes):
    return pl.pallas_call(
        plane_kernel,
        out_shape=(
            jax.ShapeDtypeStruct((FULL, LANES), jnp.float32),
            jax.ShapeDtypeStruct((planes, FULL, LANES), jnp.bfloat16),
        ),
        in_specs=[SMEM, VMEM],
        out_specs=(VMEM, VMEM),
        compiler_params=pltpu.CompilerParams(vmem_limit_bytes=8 * MIB),
        name="plane",
    )(where, pieces)


def entered(where_ref, planes_ref, inside_ref):
    before = inside_ref[0:DENSE, :]
    for k in range(planes_ref.shape[0]):
        piece = planes_ref[k, 0:DENSE, :].astype(jnp.float32)
        before = before + jnp.where(k < where_ref[2], piece, 0.0)
    return before


def advance_kernel(
    where_ref, planes_ref, inside_ref, drift_ref, noise_ref, reached_ref, state_ref, tokens_ref
):
    before = entered(where_ref, planes_ref, inside_ref)
    reached_ref[...] = before + drift_ref[...]
    beside = inside_ref[DENSE:FULL, :]
    for k in range(planes_ref.shape[0]):
        found = jnp.logical_and(where_ref[1] == 0, k == where_ref[2] - 1)
        beside = jnp.where(found, planes_ref[k, DENSE:FULL, :].astype(jnp.float32), beside)
    mixing = jnp.sum(beside, axis=0, keepdims=True)
    start = pl.multiple_of(where_ref[0] * DENSE, DENSE)
    state = noise_ref[pl.ds(start, DENSE), :] + (1.0 + mixing) * before
    state_ref[...] = state
    tokens_ref[...] = state.astype(jnp.bfloat16)


def advance(where, planes, inside, drift, noise):
    field = jax.ShapeDtypeStruct((DENSE, LANES), jnp.float32)
    return pl.pallas_call(
        advance_kernel,
        out_shape=(field, field, jax.ShapeDtypeStruct((DENSE, LANES), jnp.bfloat16)),
        in_specs=[SMEM] + [VMEM] * 4,
        out_specs=(VMEM, VMEM, VMEM),
        compiler_params=pltpu.CompilerParams(vmem_limit_bytes=8 * MIB),
        name="advance",
    )(where, planes, inside, drift, noise)


def close_kernel(
    where_ref, mixing_ref, planes_ref, inside_ref, drift_ref, noise_ref, first_ref, packed_ref
):
    reached = entered(where_ref, planes_ref, inside_ref) + drift_ref[...]
    first = first_ref[...]
    start = pl.multiple_of(where_ref[0] * DENSE, DENSE)
    packed_ref[0:DENSE, :] = (
        noise_ref[pl.ds(start, DENSE), :] + reached + mixing_ref[1, 0] * (reached - first)
    )
    missed = reached - (1.0 + mixing_ref[0, 0]) * first

    def total(values):
        return jnp.sum(jnp.sum(values * values, axis=1, keepdims=True), axis=0, keepdims=True)

    row = lax.broadcasted_iota(jnp.int32, (EXTRA, LANES), 0)
    packed_ref[DENSE:FULL, :] = jnp.where(row == 0, total(first), total(missed)) / (
        2 * DENSE * LANES
    )


def close(where, mixing, planes, inside, drift, noise, first):
    return pl.pallas_call(
        close_kernel,
        out_shape=jax.ShapeDtypeStruct((FULL, LANES), jnp.float32),
        in_specs=[SMEM] * 2 + [VMEM] * 5,
        out_specs=VMEM,
        compiler_params=pltpu.CompilerParams(vmem_limit_bytes=8 * MIB),
        name="close",
    )(where, mixing, planes, inside, drift, noise, first)


def exchanged(copies, axis):
    return lax.all_to_all(copies, axis, split_axis=0, concat_axis=0, tiled=True)


def per_device(
    noise_start,
    timesteps,
    class_labels,
    mixing,
    class_table,
    time_in,
    time_out,
    ada_weight,
    final_ada,
    patch_weight,
    q_weight,
    kv_weight,
    out_weight,
    up_weight,
    down_weight,
    final_weight,
):
    swap = [(0, 1), (1, 0)]
    up_other = lax.ppermute(up_weight, "tensor", swap)
    down_other = lax.ppermute(down_weight, "tensor", swap)
    where = jnp.stack(
        [lax.axis_index(axis) for axis in ("tensor", PLANE, "tm_0", TM)]
    ).astype(jnp.int32)
    noise = noise_start.reshape(2 * DENSE, LANES)
    modul, coefs, tokens = condition(
        where,
        timesteps,
        class_labels,
        noise,
        class_table,
        time_in,
        time_out,
        ada_weight,
        final_ada,
    )
    coarse, fine = place_tables()
    weights = (coarse, fine, patch_weight, kv_weight, q_weight, out_weight, final_weight)
    weights += (up_weight, down_weight, up_other, down_other)

    def scanned(tokens, state):
        drift, payload = denoise(
            lax.axis_size(PLANE), where, mixing, tokens, state, modul, coefs, *weights
        )
        pieces = exchanged(payload, PLANE)
        inside, payload = plane(where, pieces, lax.axis_size("tm_0"))
        return drift, inside, exchanged(payload, "tm_0")

    noise_own = lax.dynamic_slice_in_dim(noise, where[0] * DENSE, DENSE, 0)
    drift, inside, planes = scanned(tokens, noise_own)
    reached, state, tokens = advance(where, planes, inside, drift, noise)
    tokens = lax.all_gather(tokens, "tensor", tiled=True)
    drift, inside, planes = scanned(tokens, state)
    packed = lax.all_gather(
        close(where, mixing, planes, inside, drift, noise, reached), "tensor"
    )
    states = packed[:, :DENSE].reshape(1, 1, 2 * DENSE * LANES)
    residuals = packed[0, DENSE : DENSE + ITERS, :1] + packed[1, DENSE : DENSE + ITERS, :1]
    return (states, residuals)


def solution(mesh):
    split = Mesh(
        mesh.devices.reshape(8, 4, 4, mesh.shape["tensor"]), ("tm_0", "tm_1", "tm_2", "tensor")
    )
    placed = (
        P(),
        P(),
        P(TM, None),
        P(None, TM),
        P(),
        P(),
        P(),
        P(),
        P(),
        P(),
        P(),
        P(),
        P(),
        P(None, "tensor"),
        P("tensor", None),
        P(),
    )
    return jax.shard_map(
        per_device,
        mesh=split,
        in_specs=placed,
        out_specs=(P(TM, None, None), P(None, TM)),
        check_vma=False,
    )
```

```python
import math

import jax
import jax.numpy as jnp
import numpy as np
from jax import lax
from jax.experimental import pallas as pl
from jax.experimental.pallas import tpu as pltpu
from jax.sharding import Mesh
from jax.sharding import PartitionSpec as P

D = 768
HEADS = 12
SEQ = 1024
PATCH = 16
FREQ = 256
ITERS = 2
FF_OWN = 1536
TM = ("tm_0", "tm_1", "tm_2")
PLANE = ("tm_1", "tm_2")

norm_eps = 1e-06
plan_steps = 1000

OWN = SEQ // 2
LANES = 128
PER_ROW = LANES // PATCH
DENSE = OWN // PER_ROW
HALF = D // 2
ROWS = 512
GROUPS = ROWS // DENSE
MLP_ROWS = 512
MLP_CHUNK = 768
EMBED_ROWS = 512
EMBED_GROUPS = EMBED_ROWS // DENSE
MIB = 1 << 20
EXTRA = 8
FULL = DENSE + EXTRA
STEP = 32
PAIRS = HEADS // 2
Q_FACTOR = math.log2(math.e) / math.sqrt(D // HEADS)


def log_table():
    levels = np.arange(plan_steps, dtype=np.float64)
    beta_values = 0.0001 + (0.02 - 0.0001) * levels / (plan_steps - 1)
    table = np.zeros((8, LANES), np.float32)
    table.reshape(-1)[:plan_steps] = np.cumsum(np.log(1.0 - beta_values))
    return table


def angle_table(width, steps, first):
    rates = np.exp(-math.log(10000.0) * np.arange(width, dtype=np.float64) / width)
    angles = np.asarray(steps, np.float64)[:, None] * rates[None, :]
    parts = [np.cos(angles), np.sin(angles)]
    if first == "sin":
        parts = parts[::-1]
    return np.concatenate(parts, axis=1).astype(np.float32)


def place_tables():
    coarse = angle_table(HALF, PER_ROW * np.arange(SEQ // PER_ROW), "sin")
    return coarse, angle_table(HALF, np.arange(PER_ROW), "sin")


def time_table():
    count = np.arange(STEP)
    return np.concatenate(
        [angle_table(FREQ // 2, STEP * count, "cos"), angle_table(FREQ // 2, count, "cos")]
    )


def normed(values, shift, scale):
    center = values - jnp.mean(values, axis=-1, keepdims=True)
    spread = jnp.mean(center * center, axis=-1, keepdims=True)
    return center * lax.rsqrt(spread + norm_eps) * (1.0 + scale) + shift


def matmul(a, b):
    return jnp.dot(a, b, preferred_element_type=jnp.float32)


VMEM = pl.BlockSpec(memory_space=pltpu.VMEM)
SMEM = pl.BlockSpec(memory_space=pltpu.SMEM)
HBM = pl.BlockSpec(memory_space=pltpu.HBM)


def condition_kernel(
    where_ref,
    timesteps_ref,
    label_ref,
    logs_hbm,
    table_hbm,
    class_hbm,
    time_in_hbm,
    time_out_hbm,
    ada_hbm,
    final_ada_hbm,
    modul_ref,
    coef_ref,
    logs,
    table,
    class_rows,
    time_in,
    time_out,
    ada,
    sems,
):
    label = label_ref[0, 0]
    block = pl.multiple_of((label // 8) * 8, 8)
    copies = [
        pltpu.make_async_copy(table_hbm, table, sems.at[0]),
        pltpu.make_async_copy(time_in_hbm, time_in, sems.at[1]),
        pltpu.make_async_copy(time_out_hbm, time_out, sems.at[2]),
        pltpu.make_async_copy(class_hbm.at[pl.ds(block, 8), :], class_rows, sems.at[3]),
        pltpu.make_async_copy(logs_hbm, logs, sems.at[4]),
    ]
    for column in range(8):
        source = ada_hbm if column < 6 else final_ada_hbm
        at = column if column < 6 else column - 6
        copies.append(
            pltpu.make_async_copy(
                source.at[:, at * D : (at + 1) * D], ada.at[column], sems.at[5 + column]
            )
        )
    for copy in copies:
        copy.start()
    point = where_ref[3]
    now, after = timesteps_ref[point], timesteps_ref[point + 1]

    copies[0].wait()
    high = table[pl.ds(now // STEP, 1), :]
    low = table[pl.ds(STEP + now % STEP, 1), :]
    half = FREQ // 2
    high_cos, high_sin, low_cos, low_sin = high[:, :half], high[:, half:], low[:, :half], low[:, half:]
    features = jnp.concatenate(
        [high_cos * low_cos - high_sin * low_sin, high_sin * low_cos + high_cos * low_sin], axis=1
    ).astype(jnp.bfloat16)
    copies[1].wait()
    time_hidden = jax.nn.silu(matmul(features, time_in[...])).astype(jnp.bfloat16)
    copies[2].wait()
    time_embed = matmul(time_hidden, time_out[...])
    copies[3].wait()
    row = lax.broadcasted_iota(jnp.int32, (8, D), 0)
    classes = jnp.sum(
        jnp.where(row == label % 8, class_rows[...].astype(jnp.float32), 0.0), axis=0, keepdims=True
    )
    summed = jax.nn.silu(time_embed + classes).astype(jnp.bfloat16)

    copies[4].wait()
    entry = lax.broadcasted_iota(jnp.int32, (8, LANES), 0) * LANES + lax.broadcasted_iota(
        jnp.int32, (8, LANES), 1
    )

    def alpha(moment):
        found = jnp.where(entry == moment, logs[...], 0.0)
        total = jnp.sum(jnp.sum(found, axis=1, keepdims=True), axis=0, keepdims=True)
        return jnp.exp(jnp.broadcast_to(total, (8, LANES)))

    alpha_now, alpha_after = alpha(now), alpha(after)
    keep = jnp.sqrt(alpha_after / alpha_now)
    coef = jnp.sqrt(1.0 - alpha_after) - jnp.sqrt(alpha_after * (1.0 - alpha_now) / alpha_now)
    coef_ref[0:8, :] = keep - 1.0
    coef_ref[8:16, :] = coef
    for column in range(8):
        copies[5 + column].wait()
        modul_ref[:, column * D : (column + 1) * D] = matmul(summed, ada[column])


def condition(where, timesteps, labels, *weights):
    return pl.pallas_call(
        condition_kernel,
        out_shape=(
            jax.ShapeDtypeStruct((1, 8 * D), jnp.float32),
            jax.ShapeDtypeStruct((16, LANES), jnp.float32),
        ),
        in_specs=[SMEM] * 3 + [HBM] * 7,
        out_specs=(VMEM, VMEM),
        scratch_shapes=[
            pltpu.VMEM((8, LANES), jnp.float32),
            pltpu.VMEM((2 * STEP, FREQ), jnp.float32),
            pltpu.VMEM((8, D), jnp.bfloat16),
            pltpu.VMEM((FREQ, D), jnp.bfloat16),
            pltpu.VMEM((D, D), jnp.bfloat16),
            pltpu.VMEM((8, D, D), jnp.bfloat16),
            pltpu.SemaphoreType.DMA((13,)),
        ],
        compiler_params=pltpu.CompilerParams(vmem_limit_bytes=62 * MIB),
        name="condition",
    )(where, timesteps, labels, log_table(), time_table(), *weights)


def denoise_kernel(
    where_ref,
    mixing_ref,
    state_ref,
    modul_ref,
    coef_ref,
    coarse_hbm,
    fine_hbm,
    patch_hbm,
    kv_hbm,
    q_hbm,
    out_hbm,
    final_hbm,
    up_a_hbm,
    down_a_hbm,
    up_b_hbm,
    down_b_hbm,
    payload_ref,
    coarse_w,
    fine_w,
    patch_w,
    kv_w,
    q_w,
    out_w,
    final_w,
    up_w,
    down_w,
    hidden_all,
    queries,
    keys,
    values,
    attended,
    scores,
    sems,
):
    sources = [coarse_hbm, fine_hbm, patch_hbm, kv_hbm, q_hbm, out_hbm, final_hbm]
    sources += [up_a_hbm, down_a_hbm, up_b_hbm, down_b_hbm]
    targets = [coarse_w, fine_w, patch_w, kv_w, q_w, out_w, final_w]
    targets += [up_w.at[0], down_w.at[0], up_w.at[1], down_w.at[1]]
    copies = [
        pltpu.make_async_copy(source, target, sems.at[at])
        for at, (source, target) in enumerate(zip(sources, targets))
    ]
    for copy in copies[:5]:
        copy.start()
    member = where_ref[0]
    mods = [modul_ref[:, i * D : (i + 1) * D] for i in range(8)]
    shift_attn, scale_attn, gate_attn, shift_mlp, scale_mlp, gate_mlp, shift_out, scale_out = mods
    dense_lane = lax.broadcasted_iota(jnp.int32, (DENSE, LANES), 1) // PATCH
    for pair in range(PAIRS):
        values[pair, :, LANES:] = jnp.ones((SEQ, LANES), jnp.bfloat16)
    for copy in copies[:3]:
        copy.wait()
    patch = jnp.concatenate([patch_w[...]] * PER_ROW, axis=0)

    def embedded(dense, coarse, first_group):
        coarse_sin, coarse_cos = coarse[:, :HALF], coarse[:, HALF:]
        pieces = []
        for group in range(first_group, first_group + EMBED_GROUPS):
            picked = jnp.where(dense_lane == group, dense, jnp.zeros_like(dense))
            fine_sin = fine_w[group : group + 1, 0:HALF]
            fine_cos = fine_w[group : group + 1, HALF:D]
            places = jnp.concatenate(
                [
                    coarse_sin * fine_cos + coarse_cos * fine_sin,
                    coarse_cos * fine_cos - coarse_sin * fine_sin,
                ],
                axis=1,
            )
            pieces.append(matmul(picked, patch) + places)
        return jnp.concatenate(pieces, axis=0)

    for half in range(2):
        start = pl.multiple_of((member if half == 0 else 1 - member) * DENSE, DENSE)
        dense = state_ref[pl.ds(start, DENSE), :].astype(jnp.bfloat16)
        coarse = coarse_w[pl.ds(start, DENSE), :]
        for block in range(OWN // EMBED_ROWS):
            low = block * EMBED_ROWS
            hidden = embedded(dense, coarse, block * EMBED_GROUPS)
            attn_in = normed(hidden, shift_attn, scale_attn).astype(jnp.bfloat16)
            if half == 0 and block == 0:
                copies[3].wait()
                copies[4].wait()
                for copy in copies[5:]:
                    copy.start()
            if half == 0:
                hidden_all[low : low + EMBED_ROWS, :] = hidden
                q = (matmul(attn_in, q_w[...]) * Q_FACTOR).astype(jnp.bfloat16)
                for pair in range(PAIRS):
                    queries[pair, low : low + EMBED_ROWS, :] = q[:, pair * LANES : (pair + 1) * LANES]
            both = matmul(attn_in, kv_w[...]).astype(jnp.bfloat16)
            at = half * OWN + low
            for pair in range(PAIRS):
                here = pair * LANES
                keys[pair, at : at + EMBED_ROWS, :] = both[:, here : here + LANES]
                values[pair, at : at + EMBED_ROWS, 0:LANES] = both[:, D + here : D + here + LANES]

    lane = lax.broadcasted_iota(jnp.int32, (ROWS, LANES), 1)

    def score(pair, block, odd, slot):
        q = queries[pair, block * ROWS : (block + 1) * ROWS, :]
        q = jnp.where((lane >= LANES // 2) == bool(odd), q, jnp.zeros_like(q))
        scores[slot] = lax.dot_general(
            q, keys[pair], (((1,), (1,)), ((), ())), preferred_element_type=jnp.float32
        )

    def weigh(pair, slot):
        s = scores[slot]
        e = jnp.exp2(s - jnp.max(s, axis=1, keepdims=True)).astype(jnp.bfloat16)
        o = matmul(e, values[pair])
        return o[:, :LANES] / o[:, LANES:]

    def over_pair(pair, carry):
        score(pair, 0, 1, 1)
        even = weigh(pair, 0)
        score(jnp.minimum(pair + 1, PAIRS - 1), 0, 0, 0)
        odd = weigh(pair, 1)
        at = pl.multiple_of(pair * LANES, LANES)
        attended[:, pl.ds(at, LANES)] = jnp.where(lane < LANES // 2, even, odd).astype(jnp.bfloat16)
        return carry

    score(0, 0, 0, 0)
    lax.fori_loop(0, PAIRS, over_pair, 0)

    eps = jnp.zeros((DENSE, LANES), jnp.float32)
    copies[5].wait()
    copies[6].wait()
    final_tiled = jnp.concatenate([final_w[...]] * PER_ROW, axis=0)
    for copy in copies[7:]:
        copy.wait()
    for block in range(OWN // MLP_ROWS):
        rows = slice(block * MLP_ROWS, (block + 1) * MLP_ROWS)
        h1 = hidden_all[rows, :] + gate_attn * matmul(attended[rows, :], out_w[...])
        mlp_in = normed(h1, shift_mlp, scale_mlp).astype(jnp.bfloat16)
        mlp_out = None
        steps = [(part, at) for part in range(2) for at in range(0, FF_OWN, MLP_CHUNK)]

        def raised(step):
            return matmul(mlp_in, up_w[step[0], :, step[1] : step[1] + MLP_CHUNK])

        ahead = raised(steps[0])
        shares = [None, None]
        for index, (part, at) in enumerate(steps):
            now = ahead
            if index + 1 < len(steps):
                ahead = raised(steps[index + 1])
            lifted = jax.nn.gelu(now, approximate=True).astype(jnp.bfloat16)
            product = matmul(lifted, down_w[part, at : at + MLP_CHUNK, :])
            shares[part] = product if shares[part] is None else shares[part] + product
        mlp_out = sum(share.astype(jnp.bfloat16).astype(jnp.float32) for share in shares)
        h2 = h1 + gate_mlp * mlp_out
        final_in = normed(h2, shift_out, scale_out).astype(jnp.bfloat16)
        predicted = lax.dot_general(
            final_in, final_tiled, (((1,), (1,)), ((), ())), preferred_element_type=jnp.float32
        )
        for group in range(MLP_ROWS // DENSE):
            eps = jnp.where(
                dense_lane == block * (MLP_ROWS // DENSE) + group,
                predicted[group * DENSE : (group + 1) * DENSE, :],
                eps,
            )
    own = state_ref[pl.ds(pl.multiple_of(member * DENSE, DENSE), DENSE), :]
    drift = coef_ref[0:1, :] * own + coef_ref[8:9, :] * eps
    mixing = jnp.full((EXTRA, LANES), mixing_ref[0, 0], jnp.float32)
    rounded = mixing.astype(jnp.bfloat16).astype(jnp.float32)
    row = lax.broadcasted_iota(jnp.int32, (EXTRA, LANES), 0)
    beside = jnp.where(row == 0, rounded, jnp.where(row == 1, mixing - rounded, 0.0))
    sent = jnp.concatenate([drift, beside], axis=0).astype(jnp.bfloat16)
    for copy in range(payload_ref.shape[0]):
        payload_ref[copy] = sent


def denoise(copies, where, mixing, state, modul, coefs, *weights):
    bf16 = jnp.bfloat16
    return pl.pallas_call(
        denoise_kernel,
        out_shape=jax.ShapeDtypeStruct((copies, FULL, LANES), bf16),
        in_specs=[SMEM] * 2 + [VMEM] * 3 + [HBM] * 11,
        out_specs=VMEM,
        scratch_shapes=[
            pltpu.VMEM((SEQ // PER_ROW, D), jnp.float32),
            pltpu.VMEM((PER_ROW, D), jnp.float32),
            pltpu.VMEM((PATCH, D), bf16),
            pltpu.VMEM((D, 2 * D), bf16),
            pltpu.VMEM((D, D), bf16),
            pltpu.VMEM((D, D), bf16),
            pltpu.VMEM((PATCH, D), bf16),
            pltpu.VMEM((2, D, FF_OWN), bf16),
            pltpu.VMEM((2, FF_OWN, D), bf16),
            pltpu.VMEM((OWN, D), jnp.float32),
            pltpu.VMEM((PAIRS, OWN, LANES), bf16),
            pltpu.VMEM((PAIRS, SEQ, LANES), bf16),
            pltpu.VMEM((PAIRS, SEQ, 2 * LANES), bf16),
            pltpu.VMEM((OWN, D), bf16),
            pltpu.VMEM((2, ROWS, SEQ), jnp.float32),
            pltpu.SemaphoreType.DMA((11,)),
        ],
        compiler_params=pltpu.CompilerParams(vmem_limit_bytes=61 * MIB),
        name="denoise",
    )(where, mixing, state, modul, coefs, *weights)


def plane_kernel(where_ref, pieces_ref, inside_ref, payload_ref):
    here = where_ref[1]
    count = pieces_ref.shape[0]
    before = jnp.zeros((DENSE, LANES), jnp.float32)
    total = before
    own = before
    beside = jnp.zeros((EXTRA, LANES), jnp.float32)
    for k in range(count):
        piece = pieces_ref[k].astype(jnp.float32)
        before = before + jnp.where(k < here, piece[:DENSE], 0.0)
        own = jnp.where(k == here, piece[:DENSE], own)
        total = total + piece[:DENSE]
        beside = jnp.where(k == here - 1, piece[DENSE:], beside)
    inside_ref[0:DENSE, :] = before
    inside_ref[DENSE:FULL, :] = beside
    inside_ref[FULL:, :] = own
    last = pieces_ref[count - 1, DENSE:FULL, :].astype(jnp.float32)
    sent = jnp.concatenate([total, last], axis=0).astype(jnp.bfloat16)
    for copy in range(payload_ref.shape[0]):
        payload_ref[copy] = sent


def plane(where, pieces, planes):
    return pl.pallas_call(
        plane_kernel,
        out_shape=(
            jax.ShapeDtypeStruct((FULL + DENSE, LANES), jnp.float32),
            jax.ShapeDtypeStruct((planes, FULL, LANES), jnp.bfloat16),
        ),
        in_specs=[SMEM, VMEM],
        out_specs=(VMEM, VMEM),
        compiler_params=pltpu.CompilerParams(vmem_limit_bytes=8 * MIB),
        name="plane",
    )(where, pieces)


def entered(where_ref, planes_ref, inside_ref):
    before = inside_ref[0:DENSE, :]
    for k in range(planes_ref.shape[0]):
        piece = planes_ref[k, 0:DENSE, :].astype(jnp.float32)
        before = before + jnp.where(k < where_ref[2], piece, 0.0)
    return before


def advance_kernel(
    where_ref, planes_ref, inside_ref, noise_ref, reached_ref, state_ref
):
    before = entered(where_ref, planes_ref, inside_ref)
    reached_ref[...] = before + inside_ref[FULL:, :]
    beside = inside_ref[DENSE:FULL, :]
    for k in range(planes_ref.shape[0]):
        found = jnp.logical_and(where_ref[1] == 0, k == where_ref[2] - 1)
        beside = jnp.where(found, planes_ref[k, DENSE:FULL, :].astype(jnp.float32), beside)
    mixing = jnp.sum(beside, axis=0, keepdims=True)
    start = pl.multiple_of(where_ref[0] * DENSE, DENSE)
    state_ref[...] = noise_ref[pl.ds(start, DENSE), :] + (1.0 + mixing) * before


def advance(where, planes, inside, noise):
    field = jax.ShapeDtypeStruct((DENSE, LANES), jnp.float32)
    return pl.pallas_call(
        advance_kernel,
        out_shape=(field, field),
        in_specs=[SMEM] + [VMEM] * 3,
        out_specs=(VMEM, VMEM),
        compiler_params=pltpu.CompilerParams(vmem_limit_bytes=8 * MIB),
        name="advance",
    )(where, planes, inside, noise)


def close_kernel(
    where_ref, mixing_ref, planes_ref, inside_ref, noise_ref, first_ref, packed_ref
):
    reached = entered(where_ref, planes_ref, inside_ref) + inside_ref[FULL:, :]
    first = first_ref[...]
    start = pl.multiple_of(where_ref[0] * DENSE, DENSE)
    packed_ref[0:DENSE, :] = (
        noise_ref[pl.ds(start, DENSE), :] + reached + mixing_ref[0, 1] * (reached - first)
    )
    missed = reached - (1.0 + mixing_ref[0, 0]) * first

    def total(values):
        return jnp.sum(jnp.sum(values * values, axis=1, keepdims=True), axis=0, keepdims=True)

    row = lax.broadcasted_iota(jnp.int32, (EXTRA, LANES), 0)
    packed_ref[DENSE:FULL, :] = jnp.where(row == 0, total(first), total(missed)) / (
        2 * DENSE * LANES
    )


def close(where, mixing, planes, inside, noise, first):
    return pl.pallas_call(
        close_kernel,
        out_shape=jax.ShapeDtypeStruct((FULL, LANES), jnp.float32),
        in_specs=[SMEM] * 2 + [VMEM] * 4,
        out_specs=VMEM,
        compiler_params=pltpu.CompilerParams(vmem_limit_bytes=8 * MIB),
        name="close",
    )(where, mixing, planes, inside, noise, first)


def exchanged(copies, axis):
    return lax.all_to_all(copies, axis, split_axis=0, concat_axis=0, tiled=True)


def per_device(
    noise_start,
    timesteps,
    class_labels,
    mixing,
    class_table,
    time_in,
    time_out,
    ada_weight,
    final_ada,
    patch_weight,
    q_weight,
    kv_weight,
    out_weight,
    up_weight,
    down_weight,
    final_weight,
):
    swap = [(0, 1), (1, 0)]
    up_other = lax.ppermute(up_weight, "tensor", swap)
    down_other = lax.ppermute(down_weight, "tensor", swap)
    where = jnp.stack(
        [lax.axis_index(axis) for axis in ("tensor", PLANE, "tm_0", TM)]
    ).astype(jnp.int32)
    noise = noise_start.reshape(2 * DENSE, LANES)
    modul, coefs = condition(
        where,
        timesteps,
        class_labels,
        class_table,
        time_in,
        time_out,
        ada_weight,
        final_ada,
    )
    coarse, fine = place_tables()
    weights = (coarse, fine, patch_weight, kv_weight, q_weight, out_weight, final_weight.T)
    weights += (up_weight, down_weight, up_other, down_other)

    mixing = mixing.T

    def scanned(state):
        payload = denoise(lax.axis_size(PLANE), where, mixing, state, modul, coefs, *weights)
        pieces = exchanged(payload, PLANE)
        inside, payload = plane(where, pieces, lax.axis_size("tm_0"))
        return inside, exchanged(payload, "tm_0")

    inside, planes = scanned(noise)
    reached, state = advance(where, planes, inside, noise)
    state = lax.all_gather(state, "tensor", tiled=True)
    inside, planes = scanned(state)
    packed = lax.all_gather(close(where, mixing, planes, inside, noise, reached), "tensor")
    states = packed[:, :DENSE].reshape(1, 1, 2 * DENSE * LANES)
    residuals = packed[0, DENSE : DENSE + ITERS, :1] + packed[1, DENSE : DENSE + ITERS, :1]
    return (states, residuals)


def solution(mesh):
    split = Mesh(
        mesh.devices.reshape(8, 4, 4, mesh.shape["tensor"]), ("tm_0", "tm_1", "tm_2", "tensor")
    )
    placed = (
        P(),
        P(),
        P(TM, None),
        P(None, TM),
        P(),
        P(),
        P(),
        P(),
        P(),
        P(),
        P(),
        P(),
        P(),
        P(None, "tensor"),
        P("tensor", None),
        P(),
    )
    return jax.shard_map(
        per_device,
        mesh=split,
        in_specs=placed,
        out_specs=(P(TM, None, None), P(None, TM)),
        check_vma=False,
    )
```

```python
import math

import jax
import jax.numpy as jnp
import numpy as np
from jax import lax
from jax.experimental import pallas as pl
from jax.experimental.pallas import tpu as pltpu
from jax.sharding import Mesh
from jax.sharding import PartitionSpec as P

D = 768
HEADS = 12
SEQ = 1024
PATCH = 16
FREQ = 256
ITERS = 2
FF_OWN = 1536
TM = ("tm_0", "tm_1", "tm_2")
PLANE = ("tm_1", "tm_2")

norm_eps = 1e-06
plan_steps = 1000

OWN = SEQ // 2
LANES = 128
PER_ROW = LANES // PATCH
DENSE = OWN // PER_ROW
HALF = D // 2
ROWS = 512
GROUPS = ROWS // DENSE
MLP_ROWS = 512
MLP_CHUNK = 768
EMBED_ROWS = 512
EMBED_GROUPS = EMBED_ROWS // DENSE
MIB = 1 << 20
EXTRA = 8
FULL = DENSE + EXTRA
STEP = 32
PAIRS = HEADS // 2
Q_FACTOR = math.log2(math.e) / math.sqrt(D // HEADS)


def log_table():
    levels = np.arange(plan_steps, dtype=np.float64)
    beta_values = 0.0001 + (0.02 - 0.0001) * levels / (plan_steps - 1)
    table = np.zeros((8, LANES), np.float32)
    table.reshape(-1)[:plan_steps] = np.cumsum(np.log(1.0 - beta_values))
    return table


def angle_table(width, steps, first):
    rates = np.exp(-math.log(10000.0) * np.arange(width, dtype=np.float64) / width)
    angles = np.asarray(steps, np.float64)[:, None] * rates[None, :]
    parts = [np.cos(angles), np.sin(angles)]
    if first == "sin":
        parts = parts[::-1]
    return np.concatenate(parts, axis=1).astype(np.float32)


def place_tables():
    coarse = angle_table(HALF, PER_ROW * np.arange(SEQ // PER_ROW), "sin")
    return coarse, angle_table(HALF, np.arange(PER_ROW), "sin")


def time_table():
    count = np.arange(STEP)
    return np.concatenate(
        [angle_table(FREQ // 2, STEP * count, "cos"), angle_table(FREQ // 2, count, "cos")]
    )


def normed(values, shift, scale):
    center = values - jnp.mean(values, axis=-1, keepdims=True)
    spread = jnp.mean(center * center, axis=-1, keepdims=True)
    return center * lax.rsqrt(spread + norm_eps) * (1.0 + scale) + shift


def matmul(a, b):
    return jnp.dot(a, b, preferred_element_type=jnp.float32)


VMEM = pl.BlockSpec(memory_space=pltpu.VMEM)
SMEM = pl.BlockSpec(memory_space=pltpu.SMEM)
HBM = pl.BlockSpec(memory_space=pltpu.HBM)


def condition_kernel(
    where_ref,
    timesteps_ref,
    label_ref,
    logs_hbm,
    table_hbm,
    class_hbm,
    time_in_hbm,
    time_out_hbm,
    ada_hbm,
    final_ada_hbm,
    modul_ref,
    coef_ref,
    logs,
    table,
    class_rows,
    time_in,
    time_out,
    ada,
    sems,
):
    label = label_ref[0, 0]
    block = pl.multiple_of((label // 8) * 8, 8)
    copies = [
        pltpu.make_async_copy(table_hbm, table, sems.at[0]),
        pltpu.make_async_copy(time_in_hbm, time_in, sems.at[1]),
        pltpu.make_async_copy(time_out_hbm, time_out, sems.at[2]),
        pltpu.make_async_copy(class_hbm.at[pl.ds(block, 8), :], class_rows, sems.at[3]),
        pltpu.make_async_copy(logs_hbm, logs, sems.at[4]),
    ]
    for column in range(8):
        source = ada_hbm if column < 6 else final_ada_hbm
        at = column if column < 6 else column - 6
        copies.append(
            pltpu.make_async_copy(
                source.at[:, at * D : (at + 1) * D], ada.at[column], sems.at[5 + column]
            )
        )
    for copy in copies:
        copy.start()
    point = where_ref[3]
    now, after = timesteps_ref[point], timesteps_ref[point + 1]

    copies[0].wait()
    high = table[pl.ds(now // STEP, 1), :]
    low = table[pl.ds(STEP + now % STEP, 1), :]
    half = FREQ // 2
    high_cos, high_sin, low_cos, low_sin = high[:, :half], high[:, half:], low[:, :half], low[:, half:]
    features = jnp.concatenate(
        [high_cos * low_cos - high_sin * low_sin, high_sin * low_cos + high_cos * low_sin], axis=1
    ).astype(jnp.bfloat16)
    copies[1].wait()
    time_hidden = jax.nn.silu(matmul(features, time_in[...])).astype(jnp.bfloat16)
    copies[2].wait()
    time_embed = matmul(time_hidden, time_out[...])
    copies[3].wait()
    row = lax.broadcasted_iota(jnp.int32, (8, D), 0)
    classes = jnp.sum(
        jnp.where(row == label % 8, class_rows[...].astype(jnp.float32), 0.0), axis=0, keepdims=True
    )
    summed = jax.nn.silu(time_embed + classes).astype(jnp.bfloat16)

    copies[4].wait()
    entry = lax.broadcasted_iota(jnp.int32, (8, LANES), 0) * LANES + lax.broadcasted_iota(
        jnp.int32, (8, LANES), 1
    )

    def alpha(moment):
        found = jnp.where(entry == moment, logs[...], 0.0)
        total = jnp.sum(jnp.sum(found, axis=1, keepdims=True), axis=0, keepdims=True)
        return jnp.exp(jnp.broadcast_to(total, (8, LANES)))

    alpha_now, alpha_after = alpha(now), alpha(after)
    keep = jnp.sqrt(alpha_after / alpha_now)
    coef = jnp.sqrt(1.0 - alpha_after) - jnp.sqrt(alpha_after * (1.0 - alpha_now) / alpha_now)
    coef_ref[0:8, :] = keep - 1.0
    coef_ref[8:16, :] = coef
    for column in range(8):
        copies[5 + column].wait()
        modul_ref[:, column * D : (column + 1) * D] = matmul(summed, ada[column])


def condition(where, timesteps, labels, *weights):
    return pl.pallas_call(
        condition_kernel,
        out_shape=(
            jax.ShapeDtypeStruct((1, 8 * D), jnp.float32),
            jax.ShapeDtypeStruct((16, LANES), jnp.float32),
        ),
        in_specs=[SMEM] * 3 + [HBM] * 7,
        out_specs=(VMEM, VMEM),
        scratch_shapes=[
            pltpu.VMEM((8, LANES), jnp.float32),
            pltpu.VMEM((2 * STEP, FREQ), jnp.float32),
            pltpu.VMEM((8, D), jnp.bfloat16),
            pltpu.VMEM((FREQ, D), jnp.bfloat16),
            pltpu.VMEM((D, D), jnp.bfloat16),
            pltpu.VMEM((8, D, D), jnp.bfloat16),
            pltpu.SemaphoreType.DMA((13,)),
        ],
        compiler_params=pltpu.CompilerParams(vmem_limit_bytes=62 * MIB),
        name="condition",
    )(where, timesteps, labels, log_table(), time_table(), *weights)


def denoise_kernel(
    where_ref,
    mixing_ref,
    state_ref,
    modul_ref,
    coef_ref,
    coarse_hbm,
    fine_hbm,
    patch_hbm,
    kv_hbm,
    q_hbm,
    out_hbm,
    final_hbm,
    up_a_hbm,
    down_a_hbm,
    up_b_hbm,
    down_b_hbm,
    payload_ref,
    coarse_w,
    fine_w,
    patch_w,
    kv_w,
    q_w,
    out_w,
    final_w,
    up_w,
    down_w,
    hidden_all,
    queries,
    keys,
    values,
    attended,
    scores,
    sems,
):
    sources = [coarse_hbm, fine_hbm, patch_hbm, kv_hbm, q_hbm, out_hbm, final_hbm]
    sources += [up_a_hbm, down_a_hbm, up_b_hbm, down_b_hbm]
    targets = [coarse_w, fine_w, patch_w, kv_w, q_w, out_w, final_w]
    targets += [up_w.at[0], down_w.at[0], up_w.at[1], down_w.at[1]]
    copies = [
        pltpu.make_async_copy(source, target, sems.at[at])
        for at, (source, target) in enumerate(zip(sources, targets))
    ]
    for copy in copies[:5]:
        copy.start()
    member = where_ref[0]
    mods = [modul_ref[:, i * D : (i + 1) * D] for i in range(8)]
    shift_attn, scale_attn, gate_attn, shift_mlp, scale_mlp, gate_mlp, shift_out, scale_out = mods
    dense_lane = lax.broadcasted_iota(jnp.int32, (DENSE, LANES), 1) // PATCH
    for pair in range(PAIRS):
        values[pair, :, LANES:] = jnp.ones((SEQ, LANES), jnp.bfloat16)
    for copy in copies[:3]:
        copy.wait()
    patch = jnp.concatenate([patch_w[...]] * PER_ROW, axis=0)

    def embedded(dense, coarse, first_group):
        coarse_sin, coarse_cos = coarse[:, :HALF], coarse[:, HALF:]
        pieces = []
        for group in range(first_group, first_group + EMBED_GROUPS):
            picked = jnp.where(dense_lane == group, dense, jnp.zeros_like(dense))
            fine_sin = fine_w[group : group + 1, 0:HALF]
            fine_cos = fine_w[group : group + 1, HALF:D]
            places = jnp.concatenate(
                [
                    coarse_sin * fine_cos + coarse_cos * fine_sin,
                    coarse_cos * fine_cos - coarse_sin * fine_sin,
                ],
                axis=1,
            )
            pieces.append(matmul(picked, patch) + places)
        return jnp.concatenate(pieces, axis=0)

    for half in range(2):
        start = pl.multiple_of((member if half == 0 else 1 - member) * DENSE, DENSE)
        dense = state_ref[pl.ds(start, DENSE), :].astype(jnp.bfloat16)
        coarse = coarse_w[pl.ds(start, DENSE), :]
        for block in range(OWN // EMBED_ROWS):
            low = block * EMBED_ROWS
            hidden = embedded(dense, coarse, block * EMBED_GROUPS)
            attn_in = normed(hidden, shift_attn, scale_attn).astype(jnp.bfloat16)
            if half == 0 and block == 0:
                copies[3].wait()
                copies[4].wait()
                for copy in copies[5:]:
                    copy.start()
            if half == 0:
                hidden_all[low : low + EMBED_ROWS, :] = hidden
                q = (matmul(attn_in, q_w[...]) * Q_FACTOR).astype(jnp.bfloat16)
                for pair in range(PAIRS):
                    queries[pair, low : low + EMBED_ROWS, :] = q[:, pair * LANES : (pair + 1) * LANES]
            both = matmul(attn_in, kv_w[...]).astype(jnp.bfloat16)
            at = half * OWN + low
            for pair in range(PAIRS):
                here = pair * LANES
                keys[pair, at : at + EMBED_ROWS, :] = both[:, here : here + LANES]
                values[pair, at : at + EMBED_ROWS, 0:LANES] = both[:, D + here : D + here + LANES]

    lane = lax.broadcasted_iota(jnp.int32, (ROWS, LANES), 1)

    def score(pair, block, odd, slot):
        q = queries[pair, block * ROWS : (block + 1) * ROWS, :]
        q = jnp.where((lane >= LANES // 2) == bool(odd), q, jnp.zeros_like(q))
        scores[slot] = lax.dot_general(
            q, keys[pair], (((1,), (1,)), ((), ())), preferred_element_type=jnp.float32
        )

    def weigh(pair, slot):
        s = scores[slot]
        e = jnp.exp2(s - jnp.max(s, axis=1, keepdims=True)).astype(jnp.bfloat16)
        o = matmul(e, values[pair])
        return o[:, :LANES] / o[:, LANES:]

    def over_pair(pair):
        score(pair, 0, 1, 1)
        even = weigh(pair, 0)
        score(jnp.minimum(pair + 1, PAIRS - 1), 0, 0, 0)
        odd = weigh(pair, 1)
        at = pl.multiple_of(pair * LANES, LANES)
        attended[:, pl.ds(at, LANES)] = jnp.where(lane < LANES // 2, even, odd).astype(jnp.bfloat16)

    def over_pairs(step, carry):
        for inner in range(2):
            over_pair(2 * step + inner)
        return carry

    score(0, 0, 0, 0)
    lax.fori_loop(0, PAIRS // 2, over_pairs, 0)

    eps = jnp.zeros((DENSE, LANES), jnp.float32)
    copies[5].wait()
    copies[6].wait()
    final_tiled = jnp.concatenate([final_w[...]] * PER_ROW, axis=0)
    for copy in copies[7:]:
        copy.wait()
    for block in range(OWN // MLP_ROWS):
        rows = slice(block * MLP_ROWS, (block + 1) * MLP_ROWS)
        h1 = hidden_all[rows, :] + gate_attn * matmul(attended[rows, :], out_w[...])
        mlp_in = normed(h1, shift_mlp, scale_mlp).astype(jnp.bfloat16)
        mlp_out = None
        steps = [(part, at) for part in range(2) for at in range(0, FF_OWN, MLP_CHUNK)]

        def raised(step):
            return matmul(mlp_in, up_w[step[0], :, step[1] : step[1] + MLP_CHUNK])

        ahead = raised(steps[0])
        shares = [None, None]
        for index, (part, at) in enumerate(steps):
            now = ahead
            if index + 1 < len(steps):
                ahead = raised(steps[index + 1])
            lifted = jax.nn.gelu(now, approximate=True).astype(jnp.bfloat16)
            product = matmul(lifted, down_w[part, at : at + MLP_CHUNK, :])
            shares[part] = product if shares[part] is None else shares[part] + product
        mlp_out = sum(share.astype(jnp.bfloat16).astype(jnp.float32) for share in shares)
        h2 = h1 + gate_mlp * mlp_out
        final_in = normed(h2, shift_out, scale_out).astype(jnp.bfloat16)
        predicted = lax.dot_general(
            final_in, final_tiled, (((1,), (1,)), ((), ())), preferred_element_type=jnp.float32
        )
        for group in range(MLP_ROWS // DENSE):
            eps = jnp.where(
                dense_lane == block * (MLP_ROWS // DENSE) + group,
                predicted[group * DENSE : (group + 1) * DENSE, :],
                eps,
            )
    own = state_ref[pl.ds(pl.multiple_of(member * DENSE, DENSE), DENSE), :]
    drift = coef_ref[0:1, :] * own + coef_ref[8:9, :] * eps
    mixing = jnp.full((EXTRA, LANES), mixing_ref[0, 0], jnp.float32)
    rounded = mixing.astype(jnp.bfloat16).astype(jnp.float32)
    row = lax.broadcasted_iota(jnp.int32, (EXTRA, LANES), 0)
    beside = jnp.where(row == 0, rounded, jnp.where(row == 1, mixing - rounded, 0.0))
    sent = jnp.concatenate([drift, beside], axis=0).astype(jnp.bfloat16)
    for copy in range(payload_ref.shape[0]):
        payload_ref[copy] = sent


def denoise(copies, where, mixing, state, modul, coefs, *weights):
    bf16 = jnp.bfloat16
    return pl.pallas_call(
        denoise_kernel,
        out_shape=jax.ShapeDtypeStruct((copies, FULL, LANES), bf16),
        in_specs=[SMEM] * 2 + [VMEM] * 3 + [HBM] * 11,
        out_specs=VMEM,
        scratch_shapes=[
            pltpu.VMEM((SEQ // PER_ROW, D), jnp.float32),
            pltpu.VMEM((PER_ROW, D), jnp.float32),
            pltpu.VMEM((PATCH, D), bf16),
            pltpu.VMEM((D, 2 * D), bf16),
            pltpu.VMEM((D, D), bf16),
            pltpu.VMEM((D, D), bf16),
            pltpu.VMEM((PATCH, D), bf16),
            pltpu.VMEM((2, D, FF_OWN), bf16),
            pltpu.VMEM((2, FF_OWN, D), bf16),
            pltpu.VMEM((OWN, D), jnp.float32),
            pltpu.VMEM((PAIRS, OWN, LANES), bf16),
            pltpu.VMEM((PAIRS, SEQ, LANES), bf16),
            pltpu.VMEM((PAIRS, SEQ, 2 * LANES), bf16),
            pltpu.VMEM((OWN, D), bf16),
            pltpu.VMEM((2, ROWS, SEQ), jnp.float32),
            pltpu.SemaphoreType.DMA((11,)),
        ],
        compiler_params=pltpu.CompilerParams(vmem_limit_bytes=61 * MIB),
        name="denoise",
    )(where, mixing, state, modul, coefs, *weights)


def plane_kernel(where_ref, pieces_ref, inside_ref, payload_ref):
    here = where_ref[1]
    count = pieces_ref.shape[0]
    before = jnp.zeros((DENSE, LANES), jnp.float32)
    total = before
    own = before
    beside = jnp.zeros((EXTRA, LANES), jnp.float32)
    for k in range(count):
        piece = pieces_ref[k].astype(jnp.float32)
        before = before + jnp.where(k < here, piece[:DENSE], 0.0)
        own = jnp.where(k == here, piece[:DENSE], own)
        total = total + piece[:DENSE]
        beside = jnp.where(k == here - 1, piece[DENSE:], beside)
    inside_ref[0:DENSE, :] = before
    inside_ref[DENSE:FULL, :] = beside
    inside_ref[FULL:, :] = own
    last = pieces_ref[count - 1, DENSE:FULL, :].astype(jnp.float32)
    sent = jnp.concatenate([total, last], axis=0).astype(jnp.bfloat16)
    for copy in range(payload_ref.shape[0]):
        payload_ref[copy] = sent


def plane(where, pieces, planes):
    return pl.pallas_call(
        plane_kernel,
        out_shape=(
            jax.ShapeDtypeStruct((FULL + DENSE, LANES), jnp.float32),
            jax.ShapeDtypeStruct((planes, FULL, LANES), jnp.bfloat16),
        ),
        in_specs=[SMEM, VMEM],
        out_specs=(VMEM, VMEM),
        compiler_params=pltpu.CompilerParams(vmem_limit_bytes=8 * MIB),
        name="plane",
    )(where, pieces)


def entered(where_ref, planes_ref, inside_ref):
    before = inside_ref[0:DENSE, :]
    for k in range(planes_ref.shape[0]):
        piece = planes_ref[k, 0:DENSE, :].astype(jnp.float32)
        before = before + jnp.where(k < where_ref[2], piece, 0.0)
    return before


def advance_kernel(
    where_ref, planes_ref, inside_ref, noise_ref, reached_ref, state_ref
):
    before = entered(where_ref, planes_ref, inside_ref)
    reached_ref[...] = before + inside_ref[FULL:, :]
    beside = inside_ref[DENSE:FULL, :]
    for k in range(planes_ref.shape[0]):
        found = jnp.logical_and(where_ref[1] == 0, k == where_ref[2] - 1)
        beside = jnp.where(found, planes_ref[k, DENSE:FULL, :].astype(jnp.float32), beside)
    mixing = jnp.sum(beside, axis=0, keepdims=True)
    start = pl.multiple_of(where_ref[0] * DENSE, DENSE)
    state_ref[...] = noise_ref[pl.ds(start, DENSE), :] + (1.0 + mixing) * before


def advance(where, planes, inside, noise):
    field = jax.ShapeDtypeStruct((DENSE, LANES), jnp.float32)
    return pl.pallas_call(
        advance_kernel,
        out_shape=(field, field),
        in_specs=[SMEM] + [VMEM] * 3,
        out_specs=(VMEM, VMEM),
        compiler_params=pltpu.CompilerParams(vmem_limit_bytes=8 * MIB),
        name="advance",
    )(where, planes, inside, noise)


def close_kernel(
    where_ref, mixing_ref, planes_ref, inside_ref, noise_ref, first_ref, packed_ref
):
    reached = entered(where_ref, planes_ref, inside_ref) + inside_ref[FULL:, :]
    first = first_ref[...]
    start = pl.multiple_of(where_ref[0] * DENSE, DENSE)
    packed_ref[0:DENSE, :] = (
        noise_ref[pl.ds(start, DENSE), :] + reached + mixing_ref[0, 1] * (reached - first)
    )
    missed = reached - (1.0 + mixing_ref[0, 0]) * first

    def total(values):
        return jnp.sum(jnp.sum(values * values, axis=1, keepdims=True), axis=0, keepdims=True)

    row = lax.broadcasted_iota(jnp.int32, (EXTRA, LANES), 0)
    packed_ref[DENSE:FULL, :] = jnp.where(row == 0, total(first), total(missed)) / (
        2 * DENSE * LANES
    )


def close(where, mixing, planes, inside, noise, first):
    return pl.pallas_call(
        close_kernel,
        out_shape=jax.ShapeDtypeStruct((FULL, LANES), jnp.float32),
        in_specs=[SMEM] * 2 + [VMEM] * 4,
        out_specs=VMEM,
        compiler_params=pltpu.CompilerParams(vmem_limit_bytes=8 * MIB),
        name="close",
    )(where, mixing, planes, inside, noise, first)


def exchanged(copies, axis):
    return lax.all_to_all(copies, axis, split_axis=0, concat_axis=0, tiled=True)


def per_device(
    noise_start,
    timesteps,
    class_labels,
    mixing,
    class_table,
    time_in,
    time_out,
    ada_weight,
    final_ada,
    patch_weight,
    q_weight,
    kv_weight,
    out_weight,
    up_weight,
    down_weight,
    final_weight,
):
    swap = [(0, 1), (1, 0)]
    up_other = lax.ppermute(up_weight, "tensor", swap)
    down_other = lax.ppermute(down_weight, "tensor", swap)
    where = jnp.stack(
        [lax.axis_index(axis) for axis in ("tensor", PLANE, "tm_0", TM)]
    ).astype(jnp.int32)
    noise = noise_start.reshape(2 * DENSE, LANES)
    modul, coefs = condition(
        where,
        timesteps,
        class_labels,
        class_table,
        time_in,
        time_out,
        ada_weight,
        final_ada,
    )
    coarse, fine = place_tables()
    weights = (coarse, fine, patch_weight, kv_weight, q_weight, out_weight, final_weight.T)
    weights += (up_weight, down_weight, up_other, down_other)

    mixing = mixing.T

    def scanned(state):
        payload = denoise(lax.axis_size(PLANE), where, mixing, state, modul, coefs, *weights)
        pieces = exchanged(payload, PLANE)
        inside, payload = plane(where, pieces, lax.axis_size("tm_0"))
        return inside, exchanged(payload, "tm_0")

    inside, planes = scanned(noise)
    reached, state = advance(where, planes, inside, noise)
    state = lax.all_gather(state, "tensor", tiled=True)
    inside, planes = scanned(state)
    packed = lax.all_gather(close(where, mixing, planes, inside, noise, reached), "tensor")
    states = packed[:, :DENSE].reshape(1, 1, 2 * DENSE * LANES)
    residuals = jnp.sum(packed[:, DENSE : DENSE + ITERS, :1], axis=0)
    return (states, residuals)


def solution(mesh):
    split = Mesh(
        mesh.devices.reshape(8, 4, 4, mesh.shape["tensor"]), ("tm_0", "tm_1", "tm_2", "tensor")
    )
    placed = (
        P(),
        P(),
        P(TM, None),
        P(None, TM),
        P(),
        P(),
        P(),
        P(),
        P(),
        P(),
        P(),
        P(),
        P(),
        P(None, "tensor"),
        P("tensor", None),
        P(),
    )
    return jax.shard_map(
        per_device,
        mesh=split,
        in_specs=placed,
        out_specs=(P(TM, None, None), P(None, TM)),
        check_vma=False,
    )
```
